32 devices in a mesh: dp: 8 (over z, x), mp: 4 (over y, core).
Axes of the slice: x: 2, y: 2, z: 4, core: 2. Of those that a mesh axis runs over, the one named last changes fastest.
Arguments:
- media: bfloat16 [64, 256, 1536], P('dp', None, 'mp'), may hold values from -6 to 6
- time_table: bfloat16 [8, 1536], P(None, 'mp'), may hold values from -4 to 4
- doc_images: int32 [16], P('dp'), may hold values from 0 to 8, as said below
- plan: int32 [8, 8], P('dp'), may hold values from -1 to 19, as said below
- latents: bfloat16 [64, 1536], replicated, may hold values from -6 to 6
- queries: bfloat16 [64, 1024], P(None, 'mp'), may hold values from -450 to 450
- key_weight: bfloat16 [1536, 1024], P(None, 'mp'), may hold values from -0.15625 to 0.15625
- value_weight: bfloat16 [1536, 1024], P(None, 'mp'), may hold values from -0.15625 to 0.15625
- out_weight: bfloat16 [1024, 1536], P('mp'), may hold values from -0.1875 to 0.1875
- cotangent: bfloat16 [32, 64, 1536], P('dp', None, 'mp'), may hold values from -6 to 6
Outputs:
- resampled: bfloat16 [32, 64, 1536], P('dp', None, 'mp')
- key_grad: float32 [1536, 1024], P('dp', 'mp')
- value_grad: float32 [1536, 1024], P('dp', 'mp')
The draws below stay inside these ranges and needn't reach their ends.
Inputs may be any that keep to these rules, and one draw needn't show every extreme that they name: `doc_images`: A device's documents fill its image slots from slot 0 in document order and hold 8 images or fewer together; some document holds exactly 8. `plan`: entry s of device d's row is -1 exactly when slot s holds no image, else k * 4 + w with k from 0 to 4 and d + k a device of dp: the image goes to work slot w of device d + k. Each work slot receives at most one image; a device sends at most one image for each k from 1 to 4; some device sends one for every such k and fills its own 4 work slots.
All inputs are finite; a program needn't handle non-finite values.
Results may differ from the reference program's by a relative error of at most 0.0096.
Values may be sent and summed in bfloat16 or wider, within the bound.
No kernel may reach another device: no remote copies, remote signals or barrier semaphores. Data moves between devices by JAX's collectives and lax.ppermute only.
A program may use at most 64 MiB of HBM per device.

```python
import jax
import jax.numpy as jnp
from jax import lax

D = 1536
HEADS = 16
HEAD = 64
LATENTS = 64
TOKENS_IMG = 256
WORK = 4
REACH = 4
DOCS_DEV = 2
CAP = 8
INNER = 1024
SOURCES = 64
SLOTS = 32
N_DP = 8
N_MP = 4


def plan_tables(key):
    device_count = N_DP
    key_surplus, key_own, key_split = jax.random.split(jax.random.fold_in(key, 11), 3)
    raw_surplus = jax.random.randint(key_surplus, (device_count,), 0, 2 * REACH + 1)
    surplus_wish = jnp.maximum(raw_surplus - REACH, 0).astype(jnp.int32)
    own_wish = jax.random.randint(key_own, (device_count,), 0, WORK + 1).astype(jnp.int32)
    steps_back = jnp.arange(1, REACH + 1, dtype=jnp.int32)
    forced = device_count - 1 - REACH

    def advance(recent, inputs):
        index, wish, own = inputs
        incoming = jnp.sum((recent >= steps_back).astype(jnp.int32))
        quiet = (index >= forced - REACH) & (index < forced)
        surplus = jnp.where((incoming > 0) | (index >= device_count - REACH) | quiet, 0, wish)
        surplus = jnp.where(index == forced, REACH, surplus).astype(jnp.int32)
        local = jnp.where(surplus > 0, WORK, jnp.minimum(own, WORK - incoming)).astype(jnp.int32)
        recent = jnp.concatenate([surplus[None], recent[:-1]])
        return (recent, (surplus, local))
    device_iota = jnp.arange(device_count, dtype=jnp.int32)
    unused, (surplus, local) = lax.scan(advance, jnp.zeros((REACH,), jnp.int32), (device_iota, surplus_wish, own_wish))
    padded = jnp.concatenate([jnp.zeros((REACH,), jnp.int32), surplus])
    arrivals = [jnp.zeros((device_count,), jnp.int32)]
    for offset in range(1, REACH + 1):
        earlier = lax.dynamic_slice_in_dim(padded, REACH - offset, device_count)
        arrivals.append((earlier >= offset).astype(jnp.int32))
    arrive_table = jnp.stack(arrivals, 0)
    rank_table = jnp.cumsum(arrive_table, axis=0) - arrive_table
    slot_iota = jnp.arange(CAP, dtype=jnp.int32)
    far_step = (slot_iota[None, :] - WORK + 1) * jnp.ones((device_count, 1), jnp.int32)
    is_far = (far_step >= 1) & (far_step <= surplus[:, None])
    helper_index = jnp.clip(device_iota[:, None] + far_step, 0, device_count - 1)
    step_index = jnp.clip(far_step, 0, REACH)
    far_slot = local[helper_index] + rank_table[step_index, helper_index]
    is_near = slot_iota[None, :] < local[:, None]
    plan_codes = jnp.where(is_near, slot_iota[None, :], jnp.where(is_far, far_step * WORK + far_slot, -1)).astype(jnp.int32)
    loads = local + surplus
    cuts = jax.random.randint(key_split, (device_count, DOCS_DEV - 1), 0, 1 << 20) % (loads[:, None] + 1)
    cuts = jnp.where(device_iota[:, None] == forced, 0, cuts)
    cuts = jnp.sort(cuts, axis=1)
    bounds = jnp.concatenate([jnp.zeros((device_count, 1), jnp.int32), cuts.astype(jnp.int32), loads[:, None]], 1)
    counts = (bounds[:, 1:] - bounds[:, :-1]).astype(jnp.int32)
    return (counts.reshape(-1), plan_codes)


def draw_doc_images(key, part):
    counts, plan_codes = plan_tables(key)
    return counts


def draw_plan(key, part):
    counts, plan_codes = plan_tables(key)
    return plan_codes


def draw_queries(key, part):
    base = jax.random.normal(key, (LATENTS, INNER), jnp.float32)
    return jnp.clip(base, -4.0, 4.0).astype(jnp.bfloat16)


def draw_cotangent(key, part):
    sub = jax.random.fold_in(key, 23)
    base = jax.random.normal(sub, (SLOTS, LATENTS, D), jnp.float32)
    return jnp.clip(base, -6.0, 6.0).astype(jnp.bfloat16)


def raised(drawn, stream_key, source, target, parts, factor):
    owner, partner = [(jnp.arange(drawn.shape[dim]) // (drawn.shape[dim] // parts)).reshape([-1 if axis == dim else 1 for axis in range(drawn.ndim)]) for dim in (source, target)]
    chosen = jax.random.permutation(stream_key, parts)[partner]
    strong = (owner == chosen) | (owner == (partner + parts // 2) % parts)
    return jnp.where(strong, factor * drawn, drawn)


def shard_levels(key, shape, cuts, least, top_value):
    gain = 1.0
    for dim, blocks in cuts:
        heights = jax.random.uniform(jax.random.fold_in(jax.random.fold_in(key, 6), dim), (blocks,), jnp.float32, least / len(cuts), top_value / len(cuts))
        gain = gain * jnp.repeat(jnp.exp(heights), shape[dim] // blocks).reshape((-1,) + (1,) * (len(shape) - 1 - dim))
    return gain


def scatter_about(own_key, extent, deviation, most, pieces=(), held_as=jnp.bfloat16):
    drawn = deviation * jax.random.normal(own_key, extent, jnp.float32)
    if pieces:
        drawn = drawn * shard_levels(own_key, extent, pieces, -0.22, 0.18)
    return jnp.clip(drawn, -most, most).astype(held_as)


def noise_with(stream_key, extent, width, limit, pieces, heavy, kind=jnp.bfloat16):
    values = width * jax.random.normal(stream_key, extent, jnp.float32)
    if pieces:
        values = values * shard_levels(stream_key, extent, pieces, -0.22, 0.18)
    return jnp.clip(raised(values, jax.random.fold_in(stream_key, 3), *heavy), -limit, limit).astype(kind)


def setup_inputs(seed: int = 0) -> dict:
    key_of = jax.random.split(jax.random.key(seed), 11)
    return {
        "media": noise_with(key_of[0], (SOURCES, TOKENS_IMG, D), 1.0, 6.0, ((0, 8), (2, 4)), (0, 2, 8, 2.0)),
        "time_table": scatter_about(key_of[1], (CAP, D), 0.7, 4.0, ((1, 4),)),
        "doc_images": draw_doc_images(jax.random.fold_in(key_of[10], 71), 0),
        "plan": draw_plan(jax.random.fold_in(key_of[10], 71), 0),
        "latents": scatter_about(key_of[4], (LATENTS, D), 1.0, 6.0),
        "queries": draw_queries(jax.random.fold_in(key_of[10], 71), 0),
        "key_weight": scatter_about(key_of[6], (D, INNER), D ** -0.5, 0.15625, ((1, 4),)),
        "value_weight": scatter_about(key_of[7], (D, INNER), D ** -0.5, 0.15625, ((1, 4),)),
        "out_weight": scatter_about(key_of[8], (INNER, D), INNER ** -0.5, 0.1875, ((0, 4),)),
        "cotangent": draw_cotangent(jax.random.fold_in(key_of[10], 71), 0),
    }


norm_epsilon = 1e-05

def layer_norm(rows_in):
    average = lax.optimization_barrier(jnp.mean(rows_in, axis=-1, keepdims=True))
    centred = rows_in - average
    spread = lax.optimization_barrier(jnp.mean(centred * centred, axis=-1, keepdims=True))
    return centred * lax.rsqrt(spread + norm_epsilon)

def reference(media, time_table, doc_images, plan, latents, queries, key_weight, value_weight, out_weight, cotangent):
    slot_iota = jnp.arange(CAP, dtype=jnp.int32)
    counts = doc_images.reshape(N_DP, DOCS_DEV)
    doc_ends = jnp.cumsum(counts, axis=1)
    starts = doc_ends - counts
    start_of = lax.optimization_barrier(jnp.max(jnp.where(starts[:, None, :] <= slot_iota[None, :, None], starts[:, None, :], 0), axis=2))
    position = (slot_iota[None, :] - start_of).astype(jnp.int32)
    time_rows = time_table.astype(jnp.float32)[position]
    framed = (media.astype(jnp.float32).reshape(N_DP, CAP, TOKENS_IMG, D) + time_rows[:, :, None, :]).astype(jnp.bfloat16)
    is_live = plan >= 0
    helper = jnp.where(is_live, plan // WORK, 0)
    target = jnp.where(is_live, plan % WORK, 0)
    device_iota = jnp.arange(N_DP, dtype=jnp.int32)
    destination = jnp.where(is_live, (device_iota[:, None] + helper) * WORK + target, SLOTS).astype(jnp.int32).reshape(-1)
    work_media = jnp.zeros((SLOTS + 1, TOKENS_IMG, D), jnp.bfloat16).at[destination].set(framed.reshape(-1, TOKENS_IMG, D))[:SLOTS]
    alive_slot = jnp.zeros((SLOTS + 1,), jnp.float32).at[destination].set(1.0)[:SLOTS]
    latent_norm = layer_norm(latents.astype(jnp.float32)).astype(jnp.bfloat16)
    latent_keys = jnp.dot(latent_norm, key_weight, preferred_element_type=jnp.float32).astype(jnp.bfloat16)
    latent_values = jnp.dot(latent_norm, value_weight, preferred_element_type=jnp.float32).astype(jnp.bfloat16)
    query_heads = queries.astype(jnp.float32).reshape(LATENTS, HEADS, HEAD)
    group_cols = INNER // N_MP
    out_groups = out_weight.astype(jnp.float32).reshape(N_MP, group_cols, D)
    latents32 = latents.astype(jnp.float32)

    def one_slot(carry, inputs):
        key_acc, value_acc = carry
        image_rows, cot_rows, alive_one = inputs
        normed = layer_norm(image_rows.astype(jnp.float32)).astype(jnp.bfloat16)
        key_rows = jnp.concatenate([jnp.dot(normed, key_weight, preferred_element_type=jnp.float32).astype(jnp.bfloat16), latent_keys], 0)
        value_rows = jnp.concatenate([jnp.dot(normed, value_weight, preferred_element_type=jnp.float32).astype(jnp.bfloat16), latent_values], 0)
        key_heads = key_rows.astype(jnp.float32).reshape(-1, HEADS, HEAD)
        value_heads = value_rows.astype(jnp.float32).reshape(-1, HEADS, HEAD)
        scores = jnp.einsum('qhe,khe->hqk', query_heads, key_heads) * 0.125
        attention = jax.nn.softmax(scores, axis=-1)
        attention_b = attention.astype(jnp.bfloat16)
        attended = jnp.einsum('hqk,khe->qhe', attention_b.astype(jnp.float32), value_heads).reshape(LATENTS, INNER).astype(jnp.bfloat16)
        partial_g = jnp.einsum('qgc,gcd->gqd', attended.astype(jnp.float32).reshape(LATENTS, N_MP, group_cols), out_groups).astype(jnp.bfloat16)
        resampled_one = ((latents32 + lax.optimization_barrier(jnp.sum(partial_g.astype(jnp.float32), axis=0))) * alive_one).astype(jnp.bfloat16)
        cot_live = cot_rows * alive_one.astype(jnp.bfloat16)
        grad_attended = jnp.dot(cot_live, out_weight.T, preferred_element_type=jnp.float32).astype(jnp.bfloat16)
        grad_heads = grad_attended.astype(jnp.float32).reshape(LATENTS, HEADS, HEAD)
        grad_weights = jnp.einsum('qhe,khe->hqk', grad_heads, value_heads)
        row_dot = lax.optimization_barrier(jnp.sum(attention * grad_weights, axis=-1, keepdims=True))
        grad_scores = attention * (grad_weights - row_dot)
        grad_keys = (jnp.einsum('hqk,qhe->khe', grad_scores, query_heads, precision=lax.Precision.HIGHEST) * 0.125).reshape(-1, INNER).astype(jnp.bfloat16)
        grad_values = jnp.einsum('hqk,qhe->khe', attention_b.astype(jnp.float32), grad_heads).reshape(-1, INNER).astype(jnp.bfloat16)
        context = jnp.concatenate([normed, latent_norm], 0)
        key_acc = key_acc + jnp.dot(context.T, grad_keys, preferred_element_type=jnp.float32)
        value_acc = value_acc + jnp.dot(context.T, grad_values, preferred_element_type=jnp.float32)
        return ((key_acc, value_acc), resampled_one)
    start_acc = (jnp.zeros((D, INNER), jnp.float32), jnp.zeros((D, INNER), jnp.float32))
    (key_acc, value_acc), resampled = lax.scan(one_slot, start_acc, (work_media, cotangent, alive_slot))
    return (resampled, key_acc / SLOTS, value_acc / SLOTS)
```

```python
import functools

import jax
import jax.numpy as jnp
from jax import lax
from jax.experimental import pallas as pl
from jax.experimental.pallas import tpu as pltpu
from jax.sharding import PartitionSpec as P

HEAD = 64
MARK_ROWS = 16
norm_epsilon = 1e-05
f32 = jnp.float32
bf16 = jnp.bfloat16
VMEM = pl.BlockSpec(memory_space=pltpu.VMEM)
SMEM = pl.BlockSpec(memory_space=pltpu.SMEM)
ANY = pl.BlockSpec(memory_space=pl.ANY)


def from_behind(block, axis, distance):
    devices = range(lax.axis_size(axis))
    route = [(i - distance, i) for i in devices if i - distance in devices]
    return lax.ppermute(block, axis, route)


def flip(block, axis, bit):
    return lax.ppermute(block, axis, [(i, i ^ bit) for i in range(lax.axis_size(axis))])


def call(body, name, outs, in_specs, out_specs, args, scratch=(), flops=0, moved=0, limit=24, aliases=None):
    return pl.pallas_call(
        body,
        out_shape=outs,
        in_specs=in_specs,
        out_specs=out_specs,
        scratch_shapes=list(scratch),
        input_output_aliases=aliases or {},
        name=name,
        cost_estimate=pl.CostEstimate(flops=flops, bytes_accessed=moved, transcendentals=0),
        compiler_params=pltpu.CompilerParams(vmem_limit_bytes=limit << 20),
    )(*args)


def tn(a, b):
    return lax.dot_general(a, b, (((0,), (0,)), ((), ())), preferred_element_type=f32)


def nt(a, b):
    return lax.dot_general(a, b, (((1,), (1,)), ((), ())), preferred_element_type=f32)


def nn(a, b):
    return jnp.dot(a, b, preferred_element_type=f32)


def slot_position(doc_ref, slot):
    first = jnp.int32(0)
    start = jnp.int32(0)
    for j in range(doc_ref.shape[0]):
        start = jnp.where(first <= slot, jnp.maximum(start, first), start)
        first = first + doc_ref[j]
    return slot - start


def time_row(time_ref, doc_ref, slot):
    table = time_ref[...].astype(f32)
    rows = lax.broadcasted_iota(jnp.int32, table.shape, 0)
    wanted = rows == slot_position(doc_ref, slot)
    return jnp.sum(jnp.where(wanted, table, 0.0), axis=0, keepdims=True)


def prep_body(work, reach, plan_ref, doc_ref, time_ref, media_ref, *rest):
    sends = rest[:reach]
    held, sems = rest[reach:]
    tokens = media_ref.shape[1]
    chosen = []
    for k in range(1, reach + 1):
        slot = jnp.int32(0)
        mark = jnp.int32(0)
        for s in range(media_ref.shape[0]):
            code = plan_ref[0, s]
            hit = (code >= 0) & (code // work == k)
            slot = jnp.where(hit, s, slot)
            mark = jnp.where(hit, code % work + 1, mark)
        chosen.append((slot, mark))
    copies = [
        pltpu.make_async_copy(media_ref.at[chosen[k][0]], held.at[k], sems.at[k])
        for k in range(reach)
    ]
    for copy in copies:
        copy.start()
    for k in range(reach):
        slot, mark = chosen[k]
        row = time_row(time_ref, doc_ref, slot)
        sends[k][pl.ds(tokens, MARK_ROWS), :] = jnp.full(
            (MARK_ROWS, row.shape[1]), mark.astype(f32), f32
        ).astype(bf16)
        copies[k].wait()
        sends[k][pl.ds(0, tokens), :] = (held[k].astype(f32) + row).astype(bf16)


def select_body(work, reach, place, plan_ref, doc_ref, time_ref, media_ref, *rest):
    seen = min(max(reach - work + place + 1, 0), reach)
    arrivals = rest[:seen]
    out_ref, info_ref, held, sem = rest[seen:]
    slots, tokens, width = media_ref.shape
    marks = [
        jnp.max(ref[pl.ds(tokens, MARK_ROWS), pl.ds(0, 128)].astype(f32)).astype(jnp.int32)
        for ref in arrivals
    ]
    codes = [plan_ref[0, s] for s in range(slots)]
    own = [(c >= 0) & (c < work) for c in codes]
    own_count = sum(o.astype(jnp.int32) for o in own)
    taken = jnp.int32(0)
    for p in range(place + 1):
        upto = min(max(reach - work + p + 1, 0), reach)
        ready = own_count + sum([(m > 0).astype(jnp.int32) for m in marks[:upto]], jnp.int32(0))
        before = taken
        taken = jnp.minimum(taken + 1, ready)
    alive = taken > before
    rank = jnp.int32(0)
    source = jnp.int32(-1)
    target = jnp.int32(0)
    for s in range(slots):
        hit = own[s] & (rank == before) & alive
        source = jnp.where(hit, s, source)
        target = jnp.where(hit, codes[s], target)
        rank = rank + own[s].astype(jnp.int32)
    for k in range(seen):
        live = marks[k] > 0
        hit = live & (rank == before) & alive
        source = jnp.where(hit, slots + k, source)
        target = jnp.where(hit, marks[k] - 1, target)
        rank = rank + live.astype(jnp.int32)
    info_ref[0] = target
    info_ref[1] = alive.astype(jnp.int32)

    @pl.when((source >= 0) & (source < slots))
    def _():
        copy = pltpu.make_async_copy(media_ref.at[source], held, sem)
        copy.start()
        row = time_row(time_ref, doc_ref, source)
        copy.wait()
        out_ref[...] = (held[...].astype(f32) + row).astype(bf16)

    for k in range(seen):

        @pl.when(source == slots + k)
        def _():
            out_ref[...] = arrivals[k][pl.ds(0, tokens), :]

    @pl.when(source < 0)
    def _():
        out_ref[...] = jnp.zeros(out_ref.shape, bf16)


def normalise(rows):
    average = jnp.mean(rows, axis=-1, keepdims=True)
    centred = rows - average
    spread = jnp.mean(centred * centred, axis=-1, keepdims=True)
    return centred * lax.rsqrt(spread + norm_epsilon)


def own_block(shape, row_size, col_size):
    rows = lax.broadcasted_iota(jnp.int32, shape, 0) // row_size
    cols = lax.broadcasted_iota(jnp.int32, shape, 1) // col_size
    return rows == cols


def spread_heads(rows):
    heads = rows.shape[1] // HEAD
    tall = jnp.concatenate([rows.astype(f32)] * heads, axis=0)
    return jnp.where(own_block(tall.shape, rows.shape[0], HEAD), tall, 0.0)


def latent_body(latents_ref, queries_ref, kw_ref, vw_ref, norm_ref, keys_ref, values_ref, qt_ref, q_ref):
    normed = normalise(latents_ref[...].astype(f32)).astype(bf16)
    norm_ref[...] = normed
    keys_ref[...] = nn(normed, kw_ref[...]).astype(bf16)
    values_ref[...] = nn(normed, vw_ref[...]).astype(bf16)
    tall = spread_heads(queries_ref[...])
    q_ref[...] = tall.astype(bf16)
    qt_ref[...] = tall.T.astype(bf16)


def assemble(dst, blocks, parts, width):
    me = lax.axis_index("mp")
    for b in range(parts):
        start = pl.multiple_of((me ^ b) * width, width)
        dst[:, pl.ds(start, width)] = blocks[b][...]


def grad_attended_body(parts, *refs):
    blocks = refs[:parts]
    ow_ref, out_ref, full = refs[parts:]
    width = blocks[0].shape[1]
    assemble(full, blocks, parts, width)
    out_ref[...] = nt(full[...], ow_ref[...]).astype(bf16)


def place_body(parts, first, info_ref, *refs):
    blocks = refs[:parts]
    refs = refs[parts:]
    ga_ref, kw_ref, vw_ref, lk_ref, lv_ref, qt_ref, q_ref = refs[:7]
    refs = refs[7:]
    if not first:
        acc_in, lat_in = refs[:2]
        refs = refs[2:]
    acc_ref, lat_ref, att_ref, full, keys, values, grads = refs
    tokens, width = blocks[0].shape
    latents = lk_ref.shape[0]
    inner = kw_ref.shape[1]
    assemble(full, blocks, parts, width)
    x = full[...].astype(f32)
    full[...] = normalise(x).astype(bf16)
    keys[pl.ds(0, tokens), :] = nn(full[...], kw_ref[...]).astype(bf16)
    values[pl.ds(0, tokens), :] = nn(full[...], vw_ref[...]).astype(bf16)
    keys[pl.ds(tokens, latents), :] = lk_ref[...]
    values[pl.ds(tokens, latents), :] = lv_ref[...]
    scores = nn(keys[...], qt_ref[...]) * 0.125
    raised = jnp.exp(scores - jnp.max(scores, axis=0, keepdims=True))
    attention = raised / jnp.sum(raised, axis=0, keepdims=True)
    attention_b = attention.astype(bf16)
    crossed = tn(attention_b, values[...])
    crossed = jnp.where(own_block(crossed.shape, latents, HEAD), crossed, 0.0)
    heads = crossed.shape[0] // latents
    att_ref[...] = sum(crossed[h * latents : (h + 1) * latents] for h in range(heads)).astype(bf16)
    alive = info_ref[1].astype(f32)
    start = pl.multiple_of(info_ref[0] * latents, latents)
    ga = ga_ref[pl.ds(start, latents), :].astype(f32) * alive
    tall = spread_heads(ga)
    grad_weights = nn(values[...], tall.T.astype(bf16))
    row_dot = jnp.sum(attention * grad_weights, axis=0, keepdims=True)
    grad_scores = attention * (grad_weights - row_dot)
    high = grad_scores.astype(bf16)
    low = (grad_scores - high.astype(f32)).astype(bf16)
    grad_keys = ((nn(high, q_ref[...]) + nn(low, q_ref[...])) * 0.125).astype(bf16)
    grad_values = nn(attention_b, tall.astype(bf16)).astype(bf16)
    grads[:, pl.ds(0, inner)] = grad_keys[:tokens]
    grads[:, pl.ds(inner, inner)] = grad_values[:tokens]
    term = tn(full[...], grads[...])
    late_keys = grad_keys[tokens:].astype(f32)
    late_values = grad_values[tokens:].astype(f32)
    if first:
        acc_ref[...] = term
        lat_ref[:, pl.ds(0, inner)] = late_keys
        lat_ref[:, pl.ds(inner, inner)] = late_values
    else:
        acc_ref[...] = acc_in[...] + term
        lat_ref[:, pl.ds(0, inner)] = lat_in[:, pl.ds(0, inner)] + late_keys
        lat_ref[:, pl.ds(inner, inner)] = lat_in[:, pl.ds(inner, inner)] + late_values


def close_body(scale, acc_ref, lat_ref, norm_ref, key_ref, value_ref):
    inner = key_ref.shape[1]
    late = lat_ref[...]
    high = late.astype(bf16)
    low = (late - high.astype(f32)).astype(bf16)
    both = jnp.concatenate([high, low], axis=0)
    twice = jnp.concatenate([norm_ref[...]] * 2, axis=0)
    total = (acc_ref[...] + tn(twice, both)) * scale
    key_ref[...] = total[:, :inner].astype(bf16)
    value_ref[...] = total[:, inner:].astype(bf16)


def out_body(work, parts, *refs):
    infos = refs[:work]
    atts = refs[work : 2 * work]
    latents_ref, ow_ref, out_ref, base_ref, rows = refs[2 * work :]
    latents = latents_ref.shape[0]
    width = base_ref.shape[2]
    for p in range(work):
        rows[pl.ds(p * latents, latents), :] = atts[p][...]
    me = lax.axis_index("mp")
    start = pl.multiple_of(me * width, width)
    mine = latents_ref[:, pl.ds(start, width)]
    for j in range(parts):
        part = nn(rows[...], ow_ref[:, j * width : (j + 1) * width])
        for w in range(work):
            value = jnp.zeros((latents, width), f32)
            for p in range(work):
                hit = (infos[p][0] == w) & (infos[p][1] > 0)
                value = value + part[p * latents : (p + 1) * latents] * hit.astype(f32)
            out_ref[j, pl.ds(w * latents, latents), :] = value.astype(bf16)
    for w in range(work):
        live = jnp.float32(0)
        for p in range(work):
            live = live + ((infos[p][0] == w) & (infos[p][1] > 0)).astype(f32)
        base_ref[w] = mine.astype(f32) * live


def gather_blocks(block, axis):
    size = lax.axis_size(axis)
    blocks = {0: block}
    bit = size // 2
    while bit >= 1:
        for key in list(blocks):
            blocks[key ^ bit] = flip(blocks[key], axis, bit)
        bit //= 2
    return [blocks[b] for b in range(size)]


def halve(value, axis, bit_axis, bit, last=False):
    mine = (lax.axis_index(axis) // bit) % 2
    keep = lax.dynamic_index_in_dim(value, mine, bit_axis, keepdims=True)
    send = lax.dynamic_index_in_dim(value, 1 - mine, bit_axis, keepdims=True)
    got = flip(send, axis, bit)
    total = keep.astype(f32) + got.astype(f32)
    return total if last else total.astype(bf16)


def local(
    media,
    time_table,
    doc_images,
    plan,
    latents,
    queries,
    key_weight,
    value_weight,
    out_weight,
    cotangent,
):
    slots, tokens, width = media.shape
    work, latent_count, _ = cotangent.shape
    reach = slots - work
    model_width = latents.shape[1]
    inner = queries.shape[1]
    heads = inner // HEAD
    cross = heads * latent_count
    parts = lax.axis_size("mp")
    dp = lax.axis_size("dp")
    shape = jax.ShapeDtypeStruct

    sends = call(
        functools.partial(prep_body, work, reach),
        "prep",
        [shape((tokens + MARK_ROWS, width), bf16)] * reach,
        [SMEM, SMEM, VMEM, ANY],
        [VMEM] * reach,
        (plan, doc_images, time_table, media),
        [pltpu.VMEM((reach, tokens, width), bf16), pltpu.SemaphoreType.DMA((reach,))],
        moved=reach * tokens * width * 4,
    )
    arrivals = [from_behind(sends[k - 1], "dp", k) for k in range(1, reach + 1)]
    cot_blocks = gather_blocks(cotangent.reshape(work * latent_count, width), "mp")

    norm, late_keys, late_values, qt, q = call(
        latent_body,
        "latent_rows",
        [
            shape((latent_count, model_width), bf16),
            shape((latent_count, inner), bf16),
            shape((latent_count, inner), bf16),
            shape((inner, cross), bf16),
            shape((cross, inner), bf16),
        ],
        [VMEM] * 4,
        [VMEM] * 5,
        (latents, queries, key_weight, value_weight),
        flops=4 * latent_count * model_width * inner,
    )
    grad_attended = call(
        functools.partial(grad_attended_body, parts),
        "grad_attended",
        shape((work * latent_count, inner), bf16),
        [VMEM] * (parts + 1),
        VMEM,
        (*cot_blocks, out_weight),
        [pltpu.VMEM((work * latent_count, model_width), bf16)],
        flops=2 * work * latent_count * inner * model_width,
    )

    infos = []
    attended = []
    carried = ()
    for p in range(work):
        seen = min(max(reach - work + p + 1, 0), reach)
        block, info = call(
            functools.partial(select_body, work, reach, p),
            f"select_{p}",
            [shape((tokens, width), bf16), shape((2,), jnp.int32)],
            [SMEM, SMEM, VMEM, ANY] + [VMEM] * seen,
            [VMEM, SMEM],
            (plan, doc_images, time_table, media, *arrivals[:seen]),
            [pltpu.VMEM((tokens, width), bf16), pltpu.SemaphoreType.DMA],
            moved=tokens * width * 4,
        )
        infos.append(info)
        blocks = gather_blocks(block, "mp")
        first = p == 0
        count = 1 + parts + 7
        acc, lat, att = call(
            functools.partial(place_body, parts, first),
            f"place_{p}",
            [
                shape((model_width, 2 * inner), f32),
                shape((latent_count, 2 * inner), f32),
                shape((latent_count, inner), bf16),
            ],
            [SMEM] + [VMEM] * (count - 1 + len(carried)),
            [VMEM] * 3,
            (
                info,
                *blocks,
                grad_attended,
                key_weight,
                value_weight,
                late_keys,
                late_values,
                qt,
                q,
                *carried,
            ),
            [
                pltpu.VMEM((tokens, model_width), bf16),
                pltpu.VMEM((tokens + latent_count, inner), bf16),
                pltpu.VMEM((tokens + latent_count, inner), bf16),
                pltpu.VMEM((tokens, 2 * inner), bf16),
            ],
            flops=8 * tokens * model_width * inner + 14 * (tokens + latent_count) * inner * cross,
            aliases={} if first else {count: 0, count + 1: 1},
        )
        carried = (acc, lat)
        attended.append(att)

    key_part, value_part = call(
        functools.partial(close_body, 1.0 / (dp * work)),
        "close",
        [shape((model_width, inner), bf16)] * 2,
        [VMEM] * 3,
        [VMEM] * 2,
        (*carried, norm),
        flops=8 * latent_count * model_width * inner,
    )
    bits = []
    bit = 1
    while bit < dp:
        bits.append(bit)
        bit *= 2
    depth = len(bits)
    rows = model_width // dp
    key_part = key_part.reshape((2,) * depth + (rows, inner))
    value_part = value_part.reshape((2,) * depth + (rows, inner))
    turned = bits[1:] + bits[:1]
    for step in range(depth):
        last = step == depth - 1
        a, b = bits[step], turned[step]
        key_part = halve(key_part, "dp", depth - 1 - bits.index(a), a, last)
        value_part = halve(value_part, "dp", depth - 1 - bits.index(b), b, last)
    key_grad = key_part.reshape(rows, inner)
    value_grad = value_part.reshape(rows, inner)

    partial_out, base = call(
        functools.partial(out_body, work, parts),
        "out_rows",
        [
            shape((parts, work * latent_count, width), bf16),
            shape((work, latent_count, width), f32),
        ],
        [SMEM] * work + [VMEM] * (work + 2),
        [VMEM] * 2,
        (*infos, *attended, latents, out_weight),
        [pltpu.VMEM((work * latent_count, inner), bf16)],
        flops=2 * work * latent_count * inner * model_width,
    )
    mp_bits = []
    bit = 1
    while bit < parts:
        mp_bits.append(bit)
        bit *= 2
    mp_depth = len(mp_bits)
    out = partial_out.reshape((2,) * mp_depth + partial_out.shape[1:])
    for step in range(mp_depth):
        out = halve(out, "mp", mp_depth - 1 - step, mp_bits[step], step == mp_depth - 1)
    resampled = (base + out.reshape(base.shape)).astype(bf16)
    return (resampled, key_grad, value_grad)


def solution(mesh):
    return jax.shard_map(
        local,
        mesh=mesh,
        in_specs=(
            P("dp", None, "mp"),
            P(None, "mp"),
            P("dp"),
            P("dp", None),
            P(),
            P(None, "mp"),
            P(None, "mp"),
            P(None, "mp"),
            P("mp", None),
            P("dp", None, "mp"),
        ),
        out_specs=(P("dp", None, "mp"), P("dp", "mp"), P("dp", "mp")),
        check_vma=False,
    )
```

```python
import functools

import jax
import jax.numpy as jnp
from jax import lax
from jax.experimental import pallas as pl
from jax.experimental.pallas import tpu as pltpu
from jax.sharding import PartitionSpec as P


HEAD = 64
MARK_ROWS = 16
VMEM_BYTES = 67043328
norm_epsilon = 1e-05
f32 = jnp.float32
bf16 = jnp.bfloat16
VMEM = pl.BlockSpec(memory_space=pltpu.VMEM)
SMEM = pl.BlockSpec(memory_space=pltpu.SMEM)
HBM = pl.BlockSpec(memory_space=pltpu.HBM)


def from_behind(block, axis, distance):
    devices = range(lax.axis_size(axis))
    route = [(i - distance, i) for i in devices if i - distance in devices]
    return lax.ppermute(block, axis, route)


def flip(block, axis, bit):
    return lax.ppermute(block, axis, [(i, i ^ bit) for i in range(lax.axis_size(axis))])


class Chain:
    def __init__(self):
        self.token = None

    def call(
        self,
        body,
        outs,
        in_specs,
        out_specs,
        args,
        scratch=(),
        flops=0,
        moved=0,
        limit=8,
        aliases=None,
        full=False,
        spare=0,
    ):
        has = self.token is not None
        limit_bytes = limit << 20
        if full:
            held = sum(
                o.size * o.dtype.itemsize
                for o, spec in zip(outs, out_specs)
                if spec.memory_space == pltpu.VMEM
            )
            limit_bytes = VMEM_BYTES - held - spare

        def chained(*refs):
            inside = refs[has:]
            place = len(args) + len(outs)
            after = inside[place]
            after[0] = refs[0][0] if has else jnp.int32(0)
            body(*inside[:place], *inside[place + 1 :])

        *results, token = pl.pallas_call(
            chained,
            out_shape=[*outs, jax.ShapeDtypeStruct((1,), jnp.int32)],
            in_specs=[SMEM] * has + list(in_specs),
            out_specs=[*out_specs, SMEM],
            scratch_shapes=list(scratch),
            input_output_aliases={i + has: o for i, o in (aliases or {}).items()},
            cost_estimate=pl.CostEstimate(flops=flops, bytes_accessed=moved, transcendentals=0),
            compiler_params=pltpu.CompilerParams(vmem_limit_bytes=limit_bytes),
        )(*([self.token] * has), *args)
        self.token = token
        return results


def tn(a, b):
    return lax.dot_general(a, b, (((0,), (0,)), ((), ())), preferred_element_type=f32)


def nt(a, b):
    return lax.dot_general(a, b, (((1,), (1,)), ((), ())), preferred_element_type=f32)


def nn(a, b):
    return jnp.dot(a, b, preferred_element_type=f32)


def slot_position(doc_ref, slot):
    first = jnp.int32(0)
    start = jnp.int32(0)
    for j in range(doc_ref.shape[0]):
        start = jnp.where(first <= slot, jnp.maximum(start, first), start)
        first = first + doc_ref[j]
    return slot - start


def time_row(time_ref, position):
    table = time_ref[...].astype(f32)
    rows = lax.broadcasted_iota(jnp.int32, table.shape, 0)
    return jnp.sum(jnp.where(rows == position, table, 0.0), axis=0, keepdims=True)


def fetch(pairs, sems):
    copies = [pltpu.make_async_copy(src, dst, sems.at[i]) for i, (src, dst) in enumerate(pairs)]
    for copy in copies:
        copy.start()
    return copies


def prep_body(work, reach, plan_hbm, doc_hbm, time_hbm, media_ref, *rest):
    sends = rest[:reach]
    facts_ref, table_ref, held, plan_ref, doc_ref, sems, more = rest[reach:]
    slots, tokens, _ = media_ref.shape
    early = fetch([(plan_hbm, plan_ref), (doc_hbm, doc_ref), (time_hbm, table_ref)], more)
    for copy in early:
        copy.wait()
    chosen = []
    for k in range(1, reach + 1):
        slot = jnp.int32(0)
        mark = jnp.int32(0)
        for s in range(slots):
            code = plan_ref[0, s]
            hit = (code >= 0) & (code // work == k)
            slot = jnp.where(hit, s, slot)
            mark = jnp.where(hit, code % work + 1, mark)
        chosen.append((slot, mark))
    copies = fetch([(media_ref.at[slot], held.at[k]) for k, (slot, _) in enumerate(chosen)], sems)
    rank = jnp.int32(0)
    for w in range(work):
        facts_ref[w] = jnp.int32(0)
        facts_ref[work + w] = jnp.int32(0)
        facts_ref[2 * work + w] = jnp.int32(0)
    for s in range(slots):
        code = plan_ref[0, s]
        own = (code >= 0) & (code < work)

        @pl.when(own)
        def _():
            facts_ref[rank] = code
            facts_ref[work + rank] = jnp.int32(s)
            facts_ref[2 * work + rank] = slot_position(doc_ref, jnp.int32(s))

        rank = rank + own.astype(jnp.int32)
    facts_ref[3 * work] = rank
    for k in range(reach):
        slot, mark = chosen[k]
        row = time_row(table_ref, slot_position(doc_ref, slot))
        sends[k][pl.ds(tokens, MARK_ROWS), :] = jnp.full(
            (MARK_ROWS, row.shape[1]), mark.astype(f32), f32
        ).astype(bf16)
        copies[k].wait()
        sends[k][pl.ds(0, tokens), :] = (held[k].astype(f32) + row).astype(bf16)


def stage_body(work, facts_ref, table_ref, media_ref, out_ref, held, sems):
    copies = fetch(
        [(media_ref.at[facts_ref[work + w]], held.at[w]) for w in range(work)], sems
    )
    for w in range(work):
        row = time_row(table_ref, facts_ref[2 * work + w])
        copies[w].wait()
        out_ref[w] = (held[w].astype(f32) + row).astype(bf16)


def seen_at(work, reach, place):
    return min(max(reach - work + place + 1, 0), reach)


def select_body(work, reach, place, facts_ref, own_ref, *rest):
    seen = seen_at(work, reach, place)
    known = seen_at(work, reach, place - 1) if place else 0
    arrivals = rest[:seen]
    rest = rest[seen:]
    if place:
        state_in, rest = rest[0], rest[1:]
    out_ref, state_ref = rest
    tokens = out_ref.shape[0]
    own_count = facts_ref[3 * work]
    marks = [state_in[3 + k] for k in range(known)]
    for k in range(known, seen):
        mark = arrivals[k][pl.ds(tokens, MARK_ROWS), pl.ds(0, 128)].astype(f32)
        marks.append(jnp.max(mark).astype(jnp.int32))
    before = state_in[2] if place else jnp.int32(0)
    ready = own_count + sum([(m > 0).astype(jnp.int32) for m in marks], jnp.int32(0))
    alive = before < ready
    is_own = before < own_count
    index = jnp.minimum(before, work - 1)
    target = jnp.where(is_own, facts_ref[index], 0)
    source = jnp.int32(-1)
    rank = own_count
    for k in range(seen):
        live = marks[k] > 0
        hit = live & (rank == before)
        source = jnp.where(hit, k, source)
        target = jnp.where(hit, marks[k] - 1, target)
        rank = rank + live.astype(jnp.int32)
    state_ref[0] = target
    state_ref[1] = alive.astype(jnp.int32)
    state_ref[2] = before + alive.astype(jnp.int32)
    for k in range(reach):
        state_ref[3 + k] = marks[k] if k < seen else jnp.int32(0)

    @pl.when(is_own)
    def _():
        out_ref[...] = own_ref[index]

    for k in range(seen):

        @pl.when(source == k)
        def _():
            out_ref[...] = arrivals[k][pl.ds(0, tokens), :]

    @pl.when(jnp.logical_not(alive))
    def _():
        out_ref[...] = jnp.zeros(out_ref.shape, bf16)


def normalise(rows):
    average = jnp.mean(rows, axis=-1, keepdims=True)
    centred = rows - average
    spread = jnp.mean(centred * centred, axis=-1, keepdims=True)
    return centred * lax.rsqrt(spread + norm_epsilon)


def own_block(shape, row_size, col_size):
    rows = lax.broadcasted_iota(jnp.int32, shape, 0) // row_size
    cols = lax.broadcasted_iota(jnp.int32, shape, 1) // col_size
    return rows == cols


def spread_heads(rows):
    heads = rows.shape[1] // HEAD
    tall = jnp.concatenate([rows.astype(f32)] * heads, axis=0)
    return jnp.where(own_block(tall.shape, rows.shape[0], HEAD), tall, 0.0)


def latent_body(latents_ref, queries_ref, kw_ref, vw_ref, norm_ref, keys_ref, values_ref, qt_ref, q_ref):
    normed = normalise(latents_ref[...].astype(f32)).astype(bf16)
    norm_ref[...] = normed
    keys_ref[...] = nn(normed, kw_ref[...]).astype(bf16)
    values_ref[...] = nn(normed, vw_ref[...]).astype(bf16)
    tall = spread_heads(queries_ref[...])
    q_ref[...] = tall.astype(bf16)
    qt_ref[...] = tall.T.astype(bf16)


def assemble(dst, blocks, parts, width):
    me = lax.axis_index("mp")
    for b in range(parts):
        start = pl.multiple_of((me ^ b) * width, width)
        dst[:, pl.ds(start, width)] = blocks[b][...]


def grad_attended_body(parts, *refs):
    blocks = refs[:parts]
    ow_ref, out_ref, full = refs[parts:]
    width = blocks[0].shape[1]
    assemble(full, blocks, parts, width)
    out_ref[...] = nt(full[...], ow_ref[...]).astype(bf16)


def place_body(parts, first, last, scale, split, info_ref, *refs):
    blocks = refs[:parts]
    refs = refs[parts:]
    ga_ref, kw_ref, vw_ref, lk_ref, lv_ref, qt_ref, q_ref = refs[:7]
    refs = refs[7:]
    if not first:
        acc_in, lat_in = refs[:2]
        refs = refs[2:]
    if last:
        norm_ref = refs[0]
        *done, att_ref, full, keys, values, grads, late = refs[1:]
    else:
        acc_ref, lat_ref, att_ref, full, keys, values, grads = refs
    tokens, width = blocks[0].shape
    latents = lk_ref.shape[0]
    inner = kw_ref.shape[1]
    assemble(full, blocks, parts, width)
    x = full[...].astype(f32)
    full[...] = normalise(x).astype(bf16)
    keys[pl.ds(0, tokens), :] = nn(full[...], kw_ref[...]).astype(bf16)
    values[pl.ds(0, tokens), :] = nn(full[...], vw_ref[...]).astype(bf16)
    keys[pl.ds(tokens, latents), :] = lk_ref[...]
    values[pl.ds(tokens, latents), :] = lv_ref[...]
    scores = nn(keys[...], qt_ref[...]) * 0.125
    raised = jnp.exp(scores - jnp.max(scores, axis=0, keepdims=True))
    attention = raised / jnp.sum(raised, axis=0, keepdims=True)
    attention_b = attention.astype(bf16)
    crossed = tn(attention_b, values[...])
    crossed = jnp.where(own_block(crossed.shape, latents, HEAD), crossed, 0.0)
    heads = crossed.shape[0] // latents
    att_ref[...] = sum(crossed[h * latents : (h + 1) * latents] for h in range(heads)).astype(bf16)
    alive = info_ref[1].astype(f32)
    start = pl.multiple_of(info_ref[0] * latents, latents)
    ga = ga_ref[pl.ds(start, latents), :].astype(f32) * alive
    tall = spread_heads(ga)
    grad_weights = nn(values[...], tall.T.astype(bf16))
    row_dot = jnp.sum(attention * grad_weights, axis=0, keepdims=True)
    grad_scores = attention * (grad_weights - row_dot)
    high = grad_scores.astype(bf16)
    low = (grad_scores - high.astype(f32)).astype(bf16)
    grad_keys = ((nn(high, q_ref[...]) + nn(low, q_ref[...])) * 0.125).astype(bf16)
    grad_values = nn(attention_b, tall.astype(bf16)).astype(bf16)
    grads[:, pl.ds(0, inner)] = grad_keys[:tokens]
    grads[:, pl.ds(inner, inner)] = grad_values[:tokens]
    late_rows = [grad_keys[tokens:].astype(f32), grad_values[tokens:].astype(f32)]
    if not first:
        late_rows = [lat_in[:, i * inner : (i + 1) * inner] + late_rows[i] for i in range(2)]
    if not last:
        term = tn(full[...], grads[...])
        acc_ref[...] = term if first else acc_in[...] + term
        lat_ref[:, pl.ds(0, inner)] = late_rows[0]
        lat_ref[:, pl.ds(inner, inner)] = late_rows[1]
        return
    twice = jnp.concatenate([norm_ref[...]] * 2, axis=0)
    for i in range(2):
        columns = slice(i * inner, (i + 1) * inner)
        high = late_rows[i].astype(bf16)
        low = (late_rows[i] - high.astype(f32)).astype(bf16)
        total = tn(full[...], grads[:, columns]) + tn(twice, jnp.concatenate([high, low], axis=0))
        if not first:
            total = total + acc_in[:, columns]
        if split is None:
            done[i][...] = (total * scale).astype(bf16)
            continue
        rows, count, bits = split
        late[...] = total * scale
        bit = bits[i]
        mine = (lax.axis_index("dp") // bit) % 2
        for j in range(count // 2):
            for side in range(2):
                chosen = mine if side == 0 else 1 - mine
                block = (j // bit) * 2 * bit + chosen * bit + j % bit
                at = pl.multiple_of(block * rows, rows)
                done[2 * i + side][pl.ds(j * rows, rows), :] = late[pl.ds(at, rows), :].astype(bf16)


def out_body(work, parts, *refs):
    infos = refs[:work]
    atts = refs[work : 2 * work]
    latents_ref, ow_ref, out_ref, base_ref, rows = refs[2 * work :]
    latents = latents_ref.shape[0]
    width = base_ref.shape[2]
    for p in range(work):
        rows[pl.ds(p * latents, latents), :] = atts[p][...]
    me = lax.axis_index("mp")
    start = pl.multiple_of(me * width, width)
    mine = latents_ref[:, pl.ds(start, width)]
    for j in range(parts):
        part = nn(rows[...], ow_ref[:, j * width : (j + 1) * width])
        for w in range(work):
            value = jnp.zeros((latents, width), f32)
            for p in range(work):
                hit = (infos[p][0] == w) & (infos[p][1] > 0)
                value = value + part[p * latents : (p + 1) * latents] * hit.astype(f32)
            out_ref[j, pl.ds(w * latents, latents), :] = value.astype(bf16)
    for w in range(work):
        live = jnp.float32(0)
        for p in range(work):
            live = live + ((infos[p][0] == w) & (infos[p][1] > 0)).astype(f32)
        base_ref[w] = mine.astype(f32) * live


def gather_blocks(block, axis):
    size = lax.axis_size(axis)
    blocks = {0: block}
    bit = size // 2
    while bit >= 1:
        for key in list(blocks):
            blocks[key ^ bit] = flip(blocks[key], axis, bit)
        bit //= 2
    return [blocks[b] for b in range(size)]


def pick_side(value, axis, bit_axis, bit):
    mine = (lax.axis_index(axis) // bit) % 2
    keep = lax.dynamic_index_in_dim(value, mine, bit_axis, keepdims=True)
    send = lax.dynamic_index_in_dim(value, 1 - mine, bit_axis, keepdims=True)
    return keep, send


def exchange(keep, send, axis, bit, last):
    got = flip(send, axis, bit)
    total = keep.astype(f32) + got.astype(f32)
    return total if last else total.astype(bf16)


def powers(size):
    found = []
    while 2 ** len(found) < size:
        found.append(2 ** len(found))
    return found


def layer(
    media,
    time_table,
    doc_images,
    plan,
    latents,
    queries,
    key_weight,
    value_weight,
    out_weight,
    cotangent,
):
    slots, tokens, width = media.shape
    work, latent_count, _ = cotangent.shape
    reach = slots - work
    model_width = latents.shape[1]
    inner = queries.shape[1]
    heads = inner // HEAD
    cross = heads * latent_count
    parts = lax.axis_size("mp")
    dp = lax.axis_size("dp")
    bits = powers(dp)
    depth = len(bits)
    turned = bits[1:] + bits[:1]
    rows = model_width // dp
    shape = jax.ShapeDtypeStruct
    chain = Chain()

    *sends, facts, table = chain.call(
        functools.partial(prep_body, work, reach),
        [shape((tokens + MARK_ROWS, width), bf16)] * reach
        + [shape((3 * work + 1,), jnp.int32), shape(time_table.shape, bf16)],
        [HBM] * 4,
        [VMEM] * reach + [SMEM, VMEM],
        (plan, doc_images, time_table, media),
        [
            pltpu.VMEM((reach, tokens, width), bf16),
            pltpu.SMEM(plan.shape, jnp.int32),
            pltpu.SMEM(doc_images.shape, jnp.int32),
            pltpu.SemaphoreType.DMA((reach,)),
            pltpu.SemaphoreType.DMA((3,)),
        ],
        moved=reach * tokens * width * 4,
        full=True,
    )
    arrivals = []
    for k in range(1, reach + 1):
        arrivals.append(from_behind(sends[k - 1], "dp", k))
    cot_blocks = gather_blocks(cotangent.reshape(work * latent_count, width), "mp")
    (own,) = chain.call(
        functools.partial(stage_body, work),
        [shape((work, tokens, width), bf16)],
        [SMEM, VMEM, HBM],
        [VMEM],
        (facts, table, media),
        [
            pltpu.VMEM((work, tokens, width), bf16),
            pltpu.SemaphoreType.DMA((work,)),
        ],
        moved=work * tokens * width * 4,
        limit=4,
    )
    infos = []
    gathered = []
    attended = []
    carried = ()

    def select(p):
        seen = seen_at(work, reach, p)
        block, info = chain.call(
            functools.partial(select_body, work, reach, p),
            [shape((tokens, width), bf16), shape((3 + reach,), jnp.int32)],
            [SMEM] + [VMEM] * (seen + 1) + [SMEM] * (p > 0),
            [VMEM, SMEM],
            (facts, own, *arrivals[:seen], *infos[-1:]),
            moved=tokens * width * 4,
            limit=2,
        )
        infos.append(info)
        gathered.append(gather_blocks(block, "mp"))

    def place(p):
        nonlocal carried
        first, last = p == 0, p == work - 1
        count = 1 + parts + 7
        sums = [
            shape((model_width, 2 * inner), f32),
            shape((latent_count, 2 * inner), f32),
        ]
        split = None
        scratch = [
            pltpu.VMEM((tokens, model_width), bf16),
            pltpu.VMEM((tokens + latent_count, inner), bf16),
            pltpu.VMEM((tokens + latent_count, inner), bf16),
            pltpu.VMEM((tokens, 2 * inner), bf16),
        ]
        tail = ()
        if last:
            scratch.append(pltpu.VMEM((model_width, inner), f32))
            tail = (norm,)
            if rows % 16 == 0 and depth:
                split = (rows, dp, (bits[0], turned[0]))
                sums = [shape((model_width // 2, inner), bf16)] * 4
            else:
                sums = [shape((model_width, inner), bf16)] * 2
        *carried_new, att = chain.call(
            functools.partial(place_body, parts, first, last, 1.0 / (dp * work), split),
            [*sums, shape((latent_count, inner), bf16)],
            [SMEM] + [VMEM] * (count - 1 + len(carried) + len(tail)),
            [VMEM] * (len(sums) + 1),
            (
                infos[p],
                *gathered[p],
                grad_attended,
                key_weight,
                value_weight,
                late_keys,
                late_values,
                qt,
                q,
                *carried,
                *tail,
            ),
            scratch,
            flops=8 * tokens * model_width * inner + 14 * (tokens + latent_count) * inner * cross,
            limit=16,
            aliases={} if first or last else {count: 0, count + 1: 1},
        )
        carried = tuple(carried_new)
        attended.append(att)

    for p in range(work):
        select(p)
        if p == 0:
            norm, late_keys, late_values, qt, q = chain.call(
                latent_body,
                [
                    shape((latent_count, model_width), bf16),
                    shape((latent_count, inner), bf16),
                    shape((latent_count, inner), bf16),
                    shape((inner, cross), bf16),
                    shape((cross, inner), bf16),
                ],
                [VMEM] * 4,
                [VMEM] * 5,
                (latents, queries, key_weight, value_weight),
                flops=4 * latent_count * model_width * inner,
                limit=8,
            )
        if p == min(1, work - 1):
            (grad_attended,) = chain.call(
                functools.partial(grad_attended_body, parts),
                [shape((work * latent_count, inner), bf16)],
                [VMEM] * (parts + 1),
                [VMEM],
                (*cot_blocks, out_weight),
                [pltpu.VMEM((work * latent_count, model_width), bf16)],
                flops=2 * work * latent_count * inner * model_width,
                limit=8,
            )
        if p >= 2:
            place(p - 2)
    for p in range(max(work - 2, 0), work):
        place(p)

    grads = []
    for i, order in enumerate((bits, turned)):
        left = list(reversed(bits))
        if len(carried) == 4:
            keep, send = carried[2 * i : 2 * i + 2]
            left.remove(order[0])
            dims = (2,) * len(left) + (rows, inner)
            part = exchange(keep, send, "dp", order[0], depth == 1).reshape(dims)
            order = order[1:]
        else:
            part = carried[i].reshape((2,) * depth + (rows, inner))
        grads.append([part, left, order])
    for step in range(max((len(g[2]) for g in grads), default=0)):
        for g in grads:
            part, left, order = g
            bit = order[step]
            keep, send = pick_side(part, "dp", left.index(bit), bit)
            part = exchange(keep, send, "dp", bit, step == len(order) - 1)
            left.remove(bit)
            g[0] = part.reshape((2,) * len(left) + (rows, inner))
    key_grad, value_grad = [g[0].astype(f32) for g in grads]

    partial_out, base = chain.call(
        functools.partial(out_body, work, parts),
        [
            shape((parts, work * latent_count, width), bf16),
            shape((work, latent_count, width), f32),
        ],
        [SMEM] * work + [VMEM] * (work + 2),
        [VMEM] * 2,
        (*infos, *attended, latents, out_weight),
        [pltpu.VMEM((work * latent_count, inner), bf16)],
        flops=2 * work * latent_count * inner * model_width,
        limit=8,
    )
    out_bits = powers(parts)
    out = partial_out.reshape((2,) * len(out_bits) + partial_out.shape[1:])
    for step, bit in enumerate(out_bits):
        keep, send = pick_side(out, "mp", len(out_bits) - 1 - step, bit)
        out = exchange(keep, send, "mp", bit, step == len(out_bits) - 1)
    resampled = (base + out.reshape(base.shape)).astype(bf16)
    return (resampled, key_grad, value_grad)


def solution(mesh):
    return jax.shard_map(
        layer,
        mesh=mesh,
        in_specs=(
            P("dp", None, "mp"),
            P(None, "mp"),
            P("dp"),
            P("dp", None),
            P(),
            P(None, "mp"),
            P(None, "mp"),
            P(None, "mp"),
            P("mp", None),
            P("dp", None, "mp"),
        ),
        out_specs=(P("dp", None, "mp"), P("dp", "mp"), P("dp", "mp")),
        check_vma=False,
    )
```

```python
import functools

import jax
import jax.numpy as jnp
from jax import lax
from jax.experimental import pallas as pl
from jax.experimental.pallas import tpu as pltpu
from jax.sharding import PartitionSpec as P


HEAD = 64
MARK_ROWS = 16
VMEM_BYTES = 67043328
SPARE = 12000000
norm_epsilon = 1e-05
f32 = jnp.float32
bf16 = jnp.bfloat16
VMEM = pl.BlockSpec(memory_space=pltpu.VMEM)
HBM = pl.BlockSpec(memory_space=pltpu.HBM)


def from_behind(block, axis, distance):
    size = lax.axis_size(axis)
    return lax.ppermute(block, axis, [(i, (i + distance) % size) for i in range(size)])


def flip(block, axis, bit):
    return lax.ppermute(block, axis, [(i, i ^ bit) for i in range(lax.axis_size(axis))])


class Chain:
    def __init__(self):
        self.token = None

    def call(
        self,
        body,
        outs,
        in_specs,
        out_specs,
        args,
        scratch=(),
        flops=0,
        moved=0,
        limit=8,
        aliases=None,
        full=False,
        spare=0,
    ):
        has = self.token is not None
        limit_bytes = limit << 20
        if full:
            held = sum(
                o.size * o.dtype.itemsize
                for o, spec in zip(outs, out_specs)
                if spec.memory_space == pltpu.VMEM
            )
            limit_bytes = VMEM_BYTES - held - spare

        def chained(*refs):
            inside = refs[has:]
            place = len(args) + len(outs)
            inside[place][...] = jnp.zeros(inside[place].shape, f32)
            body(*inside[:place], *inside[place + 1 :])

        *results, token = pl.pallas_call(
            chained,
            out_shape=[*outs, jax.ShapeDtypeStruct((8, 128), f32)],
            in_specs=[VMEM] * has + list(in_specs),
            out_specs=[*out_specs, VMEM],
            scratch_shapes=list(scratch),
            input_output_aliases={i + has: o for i, o in (aliases or {}).items()},
            cost_estimate=pl.CostEstimate(flops=flops, bytes_accessed=moved, transcendentals=0),
            compiler_params=pltpu.CompilerParams(vmem_limit_bytes=limit_bytes),
        )(*([self.token] * has), *args)
        self.token = token
        return results


def tn(a, b):
    return lax.dot_general(a, b, (((0,), (0,)), ((), ())), preferred_element_type=f32)


def nt(a, b):
    return lax.dot_general(a, b, (((1,), (1,)), ((), ())), preferred_element_type=f32)


def nn(a, b):
    return jnp.dot(a, b, preferred_element_type=f32)


def slot_position(doc_ref, slot):
    first = jnp.int32(0)
    start = jnp.int32(0)
    for j in range(doc_ref.shape[0]):
        start = jnp.where(first <= slot, jnp.maximum(start, first), start)
        first = first + doc_ref[j]
    return slot - start


def time_row(time_ref, position):
    table = time_ref[...].astype(f32)
    rows = lax.broadcasted_iota(jnp.int32, table.shape, 0)
    return jnp.sum(jnp.where(rows == position, table, 0.0), axis=0, keepdims=True)


def fetch(pairs, sems):
    copies = [pltpu.make_async_copy(src, dst, sems.at[i]) for i, (src, dst) in enumerate(pairs)]
    for copy in copies:
        copy.start()
    return copies


def prep_body(work, reach, plan_hbm, doc_hbm, time_hbm, media_ref, *rest):
    sends = rest[:reach]
    own_ref, rows_ref, facts_ref, held, plan_ref, doc_ref, time_ref, sems, own_sems, more = rest[
        reach:
    ]
    slots, tokens, width = media_ref.shape
    early = fetch([(plan_hbm, plan_ref), (doc_hbm, doc_ref), (time_hbm, time_ref)], more)
    for copy in early:
        copy.wait()
    codes = [plan_ref[0, s] for s in range(slots)]
    chosen = []
    for k in range(1, reach + 1):
        slot = jnp.int32(0)
        mark = jnp.int32(0)
        for s in range(slots):
            hit = (codes[s] >= k * work) & (codes[s] < (k + 1) * work)
            slot = jnp.where(hit, s, slot)
            mark = jnp.where(hit, codes[s] - k * work + 1, mark)
        chosen.append((slot, mark))
    copies = fetch([(media_ref.at[slot], held.at[k]) for k, (slot, _) in enumerate(chosen)], sems)
    own_slots = [jnp.int32(0)] * work
    own_codes = [jnp.int32(0)] * work
    rank = jnp.int32(0)
    for s in range(slots):
        own = (codes[s] >= 0) & (codes[s] < work)
        for w in range(work):
            hit = own & (rank == w)
            own_slots[w] = jnp.where(hit, s, own_slots[w])
            own_codes[w] = jnp.where(hit, codes[s], own_codes[w])
        rank = rank + own.astype(jnp.int32)
    own_copies = fetch([(media_ref.at[own_slots[w]], own_ref.at[w]) for w in range(work)], own_sems)

    def splat(value):
        return jnp.full((1, width), value.astype(f32), f32)

    facts_ref[...] = jnp.zeros(facts_ref.shape, f32)
    facts_ref[pl.ds(work, 1), :] = splat(rank)
    for w in range(work):
        facts_ref[pl.ds(w, 1), :] = splat(own_codes[w])
        rows_ref[pl.ds(w, 1), :] = time_row(time_ref, slot_position(doc_ref, own_slots[w]))
    for k in range(reach):
        slot, mark = chosen[k]
        row = time_row(time_ref, slot_position(doc_ref, slot))
        sends[k][pl.ds(tokens, MARK_ROWS), :] = jnp.full(
            (MARK_ROWS, width), mark.astype(f32), f32
        ).astype(bf16)
        copies[k].wait()
        sends[k][pl.ds(0, tokens), :] = (held[k].astype(f32) + row).astype(bf16)
    for copy in own_copies:
        copy.wait()


def seen_at(work, reach, place):
    return min(max(reach - work + place + 1, 0), reach)


def select_body(work, reach, place, facts_ref, rows_ref, own_ref, *rest):
    seen = seen_at(work, reach, place)
    arrivals = rest[:seen]
    out_ref, info_ref = rest[seen:]
    tokens, width = out_ref.shape
    own_count = facts_ref[pl.ds(work, 1), :]
    marks = [ref[pl.ds(tokens, MARK_ROWS), :].astype(f32)[:1] for ref in arrivals]
    lives = [jnp.minimum(mark, 1.0) for mark in marks]
    taken = jnp.zeros((1, width), f32)
    for p in range(place + 1):
        ready = own_count
        for live in lives[: seen_at(work, reach, p)]:
            ready = ready + live
        before = taken
        taken = jnp.minimum(taken + 1.0, ready)
    alive = taken - before
    target = jnp.zeros((1, width), f32)
    row = jnp.zeros((1, width), f32)
    raw = jnp.zeros((tokens, width), bf16)
    for w in range(min(work, place + 1)):
        weight = jnp.where((before == w) & (own_count > w), 1.0, 0.0)
        target = target + weight * facts_ref[pl.ds(w, 1), :]
        row = row + weight * rows_ref[pl.ds(w, 1), :]
        raw = raw + own_ref[w] * weight.astype(bf16)
    block = (raw.astype(f32) + row).astype(bf16)
    rank = own_count
    for k in range(seen):
        weight = jnp.where(rank == before, lives[k], 0.0)
        target = target + weight * (marks[k] - 1.0)
        block = block + arrivals[k][pl.ds(0, tokens), :] * weight.astype(bf16)
        rank = rank + lives[k]
    out_ref[...] = block
    lanes = info_ref.shape[1]
    info_ref[...] = jnp.zeros(info_ref.shape, f32)
    info_ref[pl.ds(0, 1), :] = target[:, :lanes]
    info_ref[pl.ds(1, 1), :] = alive[:, :lanes]


def normalise(rows):
    average = jnp.mean(rows, axis=-1, keepdims=True)
    centred = rows - average
    spread = jnp.mean(centred * centred, axis=-1, keepdims=True)
    return centred * lax.rsqrt(spread + norm_epsilon)


def own_block(shape, row_size, col_size):
    rows = lax.broadcasted_iota(jnp.int32, shape, 0) // row_size
    cols = lax.broadcasted_iota(jnp.int32, shape, 1) // col_size
    return rows == cols


def spread_heads(rows):
    heads = rows.shape[1] // HEAD
    tall = jnp.concatenate([rows.astype(f32)] * heads, axis=0)
    return jnp.where(own_block(tall.shape, rows.shape[0], HEAD), tall, 0.0)


def assemble(dst, blocks, parts, width):
    me = lax.axis_index("mp")
    for b in range(parts):
        start = pl.multiple_of((me ^ b) * width, width)
        dst[pl.ds(0, blocks[b].shape[0]), pl.ds(start, width)] = blocks[b][...]


def slot_hit(info_ref, slot):
    target = info_ref[pl.ds(0, 1), pl.ds(0, 1)]
    return jnp.where(target == slot, info_ref[pl.ds(1, 1), pl.ds(0, 1)], 0.0)


def place_body(parts, first, last, scale, split, info_ref, *refs):
    blocks, refs = refs[:parts], refs[parts:]
    kw_ref, vw_ref, refs = refs[0], refs[1], refs[2:]
    if first:
        latents_ref, queries_ref, ow_ref, refs = *refs[:3], refs[3:]
        cots, refs = refs[:parts], refs[parts:]
        acc_ref, lat_ref, att_ref, ga_ref, lk_ref, lv_ref, qt_ref, q_ref, norm_ref, *refs = refs
        full, keys, values, grads, cot_full = refs
    else:
        acc_in, lat_in, ga_ref, lk_ref, lv_ref, qt_ref, q_ref, norm_ref, *refs = refs
        if last:
            *done, att_ref, full, keys, values, grads, late = refs
        else:
            acc_ref, lat_ref, att_ref, full, keys, values, grads = refs
    tokens, width = blocks[0].shape
    latents = lk_ref.shape[0]
    inner = kw_ref.shape[1]
    assemble(full, blocks, parts, width)
    chunk = tokens if tokens % 32 else 32
    for r in range(0, tokens, chunk):
        rows = full[pl.ds(r, chunk), :].astype(f32)
        full[pl.ds(r, chunk), :] = normalise(rows).astype(bf16)
    if first:
        assemble(cot_full, cots, parts, width)
        normed = normalise(latents_ref[...].astype(f32)).astype(bf16)
        norm_ref[...] = normed
        full[pl.ds(tokens, latents), :] = normed
        keys[...] = nn(full[...], kw_ref[...]).astype(bf16)
        values[...] = nn(full[...], vw_ref[...]).astype(bf16)
        lk_ref[...] = keys[pl.ds(tokens, latents), :]
        lv_ref[...] = values[pl.ds(tokens, latents), :]
        tall = spread_heads(queries_ref[...])
        q_ref[...] = tall.astype(bf16)
        qt_ref[...] = tall.T.astype(bf16)
        ga_ref[...] = nt(cot_full[...], ow_ref[...]).astype(bf16)
    else:
        keys[pl.ds(0, tokens), :] = nn(full[...], kw_ref[...]).astype(bf16)
        values[pl.ds(0, tokens), :] = nn(full[...], vw_ref[...]).astype(bf16)
        keys[pl.ds(tokens, latents), :] = lk_ref[...]
        values[pl.ds(tokens, latents), :] = lv_ref[...]
    scores = nn(keys[...], qt_ref[...]) * 0.125
    raised = jnp.exp(scores - jnp.max(scores, axis=0, keepdims=True))
    attention = raised / jnp.sum(raised, axis=0, keepdims=True)
    attention_b = attention.astype(bf16)
    crossed = tn(attention_b, values[...])
    crossed = jnp.where(own_block(crossed.shape, latents, HEAD), crossed, 0.0)
    heads = crossed.shape[0] // latents
    att_ref[...] = sum(crossed[h * latents : (h + 1) * latents] for h in range(heads)).astype(bf16)
    ga = jnp.zeros((latents, inner), f32)
    for w in range(ga_ref.shape[0] // latents):
        ga = ga + ga_ref[pl.ds(w * latents, latents), :].astype(f32) * slot_hit(info_ref, w)
    tall = spread_heads(ga)
    grad_weights = nn(values[...], tall.T.astype(bf16))
    row_dot = jnp.sum(attention * grad_weights, axis=0, keepdims=True)
    grad_scores = attention * (grad_weights - row_dot)
    high = grad_scores.astype(bf16)
    low = (grad_scores - high.astype(f32)).astype(bf16)
    grad_keys = ((nn(high, q_ref[...]) + nn(low, q_ref[...])) * 0.125).astype(bf16)
    grad_values = nn(attention_b, tall.astype(bf16)).astype(bf16)
    grads[:, pl.ds(0, inner)] = grad_keys[:tokens]
    grads[:, pl.ds(inner, inner)] = grad_values[:tokens]
    late_rows = [grad_keys[tokens:].astype(f32), grad_values[tokens:].astype(f32)]
    if not first:
        late_rows = [lat_in[:, i * inner : (i + 1) * inner] + late_rows[i] for i in range(2)]
    if not last:
        term = tn(full[pl.ds(0, tokens), :], grads[...])
        acc_ref[...] = term if first else acc_in[...] + term
        lat_ref[:, pl.ds(0, inner)] = late_rows[0]
        lat_ref[:, pl.ds(inner, inner)] = late_rows[1]
        return
    twice = jnp.concatenate([norm_ref[...]] * 2, axis=0)
    for i in range(2):
        columns = slice(i * inner, (i + 1) * inner)
        high = late_rows[i].astype(bf16)
        low = (late_rows[i] - high.astype(f32)).astype(bf16)
        total = tn(full[pl.ds(0, tokens), :], grads[:, columns]) + tn(twice, jnp.concatenate([high, low], axis=0))
        if not first:
            total = total + acc_in[:, columns]
        if split is None:
            done[i][...] = (total * scale).astype(bf16)
            continue
        rows, count, bits = split
        late[...] = total * scale
        bit = bits[i]
        mine = (lax.axis_index("dp") // bit) % 2
        for j in range(count // 2):
            for side in range(2):
                chosen = mine if side == 0 else 1 - mine
                block = (j // bit) * 2 * bit + chosen * bit + j % bit
                at = pl.multiple_of(block * rows, rows)
                done[2 * i + side][pl.ds(j * rows, rows), :] = late[pl.ds(at, rows), :].astype(bf16)


def out_body(work, parts, *refs):
    infos = refs[:work]
    atts = refs[work : 2 * work]
    latents_ref, ow_ref, out_ref, base_ref, rows = refs[2 * work :]
    latents = latents_ref.shape[0]
    width = base_ref.shape[2]
    for p in range(work):
        rows[pl.ds(p * latents, latents), :] = atts[p][...]
    me = lax.axis_index("mp")
    start = pl.multiple_of(me * width, width)
    mine = latents_ref[:, pl.ds(start, width)]
    for j in range(parts):
        part = nn(rows[...], ow_ref[:, j * width : (j + 1) * width])
        for w in range(work):
            value = jnp.zeros((latents, width), f32)
            for p in range(work):
                rows_p = part[p * latents : (p + 1) * latents]
                value = value + rows_p * slot_hit(infos[p], w)
            out_ref[j, pl.ds(w * latents, latents), :] = value.astype(bf16)
    for w in range(work):
        live = jnp.zeros((1, 1), f32)
        for p in range(work):
            live = live + slot_hit(infos[p], w)
        base_ref[w] = mine.astype(f32) * live


def gather_blocks(block, axis):
    size = lax.axis_size(axis)
    blocks = {0: block}
    bit = size // 2
    while bit >= 1:
        for key in list(blocks):
            blocks[key ^ bit] = flip(blocks[key], axis, bit)
        bit //= 2
    return [blocks[b] for b in range(size)]


def pick_side(value, axis, bit_axis, bit):
    mine = (lax.axis_index(axis) // bit) % 2
    keep = lax.dynamic_index_in_dim(value, mine, bit_axis, keepdims=True)
    send = lax.dynamic_index_in_dim(value, 1 - mine, bit_axis, keepdims=True)
    return keep, send


def exchange(keep, send, axis, bit, last):
    got = flip(send, axis, bit)
    total = keep.astype(f32) + got.astype(f32)
    return total if last else total.astype(bf16)


def powers(size):
    found = []
    while 2 ** len(found) < size:
        found.append(2 ** len(found))
    return found


def layer(
    media,
    time_table,
    doc_images,
    plan,
    latents,
    queries,
    key_weight,
    value_weight,
    out_weight,
    cotangent,
):
    slots, tokens, width = media.shape
    work, latent_count, _ = cotangent.shape
    reach = slots - work
    model_width = latents.shape[1]
    inner = queries.shape[1]
    heads = inner // HEAD
    cross = heads * latent_count
    parts = lax.axis_size("mp")
    dp = lax.axis_size("dp")
    bits = powers(dp)
    depth = len(bits)
    turned = bits[1:] + bits[:1]
    rows = model_width // dp
    shape = jax.ShapeDtypeStruct
    chain = Chain()

    fact_rows = -(-(work + 1) // 8) * 8
    *sends, own, own_rows, facts = chain.call(
        functools.partial(prep_body, work, reach),
        [shape((tokens + MARK_ROWS, width), bf16)] * reach
        + [
            shape((work, tokens, width), bf16),
            shape((fact_rows, width), f32),
            shape((fact_rows, width), f32),
        ],
        [HBM] * 4,
        [VMEM] * (reach + 3),
        (plan, doc_images, time_table, media),
        [
            pltpu.VMEM((reach, tokens, width), bf16),
            pltpu.SMEM(plan.shape, jnp.int32),
            pltpu.SMEM(doc_images.shape, jnp.int32),
            pltpu.VMEM(time_table.shape, bf16),
            pltpu.SemaphoreType.DMA((reach,)),
            pltpu.SemaphoreType.DMA((work,)),
            pltpu.SemaphoreType.DMA((3,)),
        ],
        moved=(reach + work) * tokens * width * 4,
        full=True,
        spare=SPARE,
    )
    arrivals = []
    for k in range(1, reach + 1):
        arrivals.append(from_behind(sends[k - 1], "dp", k))
    cot_blocks = gather_blocks(cotangent.reshape(work * latent_count, width), "mp")
    infos = []
    gathered = []
    attended = []
    sums = ()
    shared = ()

    def select(p):
        seen = seen_at(work, reach, p)
        block, info = chain.call(
            functools.partial(select_body, work, reach, p),
            [shape((tokens, width), bf16), shape((8, 128), f32)],
            [VMEM] * (seen + 3),
            [VMEM, VMEM],
            (facts, own_rows, own, *arrivals[:seen]),
            moved=tokens * width * 4,
            limit=2,
        )
        infos.append(info)
        gathered.append(gather_blocks(block, "mp"))

    def place(p):
        nonlocal sums, shared
        first, last = p == 0, p == work - 1
        held_rows = tokens + latent_count
        split = None
        new = [
            shape((model_width, 2 * inner), f32),
            shape((latent_count, 2 * inner), f32),
        ]
        if last:
            if rows % 16 == 0 and depth:
                split = (rows, dp, (bits[0], turned[0]))
                new = [shape((model_width // 2, inner), bf16)] * 4
            else:
                new = [shape((model_width, inner), bf16)] * 2
        scratch = [
            pltpu.VMEM((held_rows if first else tokens, model_width), bf16),
            pltpu.VMEM((held_rows, inner), bf16),
            pltpu.VMEM((held_rows, inner), bf16),
            pltpu.VMEM((tokens, 2 * inner), bf16),
        ]
        args = (infos[p], *gathered[p], key_weight, value_weight)
        extra = []
        if first:
            args += (latents, queries, out_weight, *cot_blocks)
            extra = [
                shape((work * latent_count, inner), bf16),
                shape((latent_count, inner), bf16),
                shape((latent_count, inner), bf16),
                shape((inner, cross), bf16),
                shape((cross, inner), bf16),
                shape((latent_count, model_width), bf16),
            ]
            scratch.append(pltpu.VMEM((work * latent_count, model_width), bf16))
        else:
            args += (*sums, *shared)
        if last:
            scratch.append(pltpu.VMEM((model_width, inner), f32))
        start = 3 + parts
        results = chain.call(
            functools.partial(place_body, parts, first, last, 1.0 / (dp * work), split),
            [*new, shape((latent_count, inner), bf16), *extra],
            [VMEM] * len(args),
            [VMEM] * (len(new) + 1 + len(extra)),
            args,
            scratch,
            flops=8 * tokens * model_width * inner + 14 * held_rows * inner * cross,
            limit=16,
            aliases={} if first or last else {start: 0, start + 1: 1},
        )
        sums = tuple(results[: len(new)])
        attended.append(results[len(new)])
        if first:
            shared = tuple(results[len(new) + 1 :])

    for p in range(work):
        if p >= 3:
            place(p - 3)
        select(p)
    for p in range(max(work - 3, 0), work):
        place(p)
    carried = sums

    grads = []
    for i, order in enumerate((bits, turned)):
        left = list(reversed(bits))
        if len(carried) == 4:
            keep, send = carried[2 * i : 2 * i + 2]
            left.remove(order[0])
            dims = (2,) * len(left) + (rows, inner)
            part = exchange(keep, send, "dp", order[0], depth == 1).reshape(dims)
            order = order[1:]
        else:
            part = carried[i].reshape((2,) * depth + (rows, inner))
        grads.append([part, left, order])
    for step in range(max((len(g[2]) for g in grads), default=0)):
        for g in grads:
            part, left, order = g
            bit = order[step]
            keep, send = pick_side(part, "dp", left.index(bit), bit)
            part = exchange(keep, send, "dp", bit, step == len(order) - 1)
            left.remove(bit)
            g[0] = part.reshape((2,) * len(left) + (rows, inner))
    key_grad, value_grad = [g[0].astype(f32) for g in grads]

    partial_out, base = chain.call(
        functools.partial(out_body, work, parts),
        [
            shape((parts, work * latent_count, width), bf16),
            shape((work, latent_count, width), f32),
        ],
        [VMEM] * (2 * work + 2),
        [VMEM] * 2,
        (*infos, *attended, latents, out_weight),
        [pltpu.VMEM((work * latent_count, inner), bf16)],
        flops=2 * work * latent_count * inner * model_width,
        limit=8,
    )
    out_bits = powers(parts)
    out = partial_out.reshape((2,) * len(out_bits) + partial_out.shape[1:])
    for step, bit in enumerate(out_bits):
        keep, send = pick_side(out, "mp", len(out_bits) - 1 - step, bit)
        out = exchange(keep, send, "mp", bit, step == len(out_bits) - 1)
    resampled = (base + out.reshape(base.shape)).astype(bf16)
    return (resampled, key_grad, value_grad)


def solution(mesh):
    return jax.shard_map(
        layer,
        mesh=mesh,
        in_specs=(
            P("dp", None, "mp"),
            P(None, "mp"),
            P("dp"),
            P("dp", None),
            P(),
            P(None, "mp"),
            P(None, "mp"),
            P(None, "mp"),
            P("mp", None),
            P("dp", None, "mp"),
        ),
        out_specs=(P("dp", None, "mp"), P("dp", "mp"), P("dp", "mp")),
        check_vma=False,
    )
```

```python
import functools

import jax
import jax.numpy as jnp
from jax import lax
from jax.experimental import pallas as pl
from jax.experimental.pallas import tpu as pltpu
from jax.sharding import PartitionSpec as P


HEAD = 64
MARK_ROWS = 8
VMEM_BYTES = 67043328
SPARE = 12000000
norm_epsilon = 1e-05
f32 = jnp.float32
bf16 = jnp.bfloat16
VMEM = pl.BlockSpec(memory_space=pltpu.VMEM)
HBM = pl.BlockSpec(memory_space=pltpu.HBM)


def from_behind(block, axis, distance):
    size = lax.axis_size(axis)
    route = [(i, (i + distance) % size) for i in range(size)]
    if distance >= 3:
        route = [(i, j) for i, j in route if j > i]
    return lax.ppermute(block, axis, route)


def flip(block, axis, bit):
    return lax.ppermute(block, axis, [(i, i ^ bit) for i in range(lax.axis_size(axis))])


class Chain:
    def __init__(self):
        self.token = None

    def call(
        self,
        body,
        outs,
        in_specs,
        out_specs,
        args,
        scratch=(),
        flops=0,
        moved=0,
        limit=8,
        aliases=None,
        full=False,
        spare=0,
    ):
        has = self.token is not None
        limit_bytes = limit << 20
        if full:
            held = sum(
                o.size * o.dtype.itemsize
                for o, spec in zip(outs, out_specs)
                if spec.memory_space == pltpu.VMEM
            )
            limit_bytes = VMEM_BYTES - held - spare

        def chained(*refs):
            inside = refs[has:]
            place = len(args) + len(outs)
            inside[place][...] = jnp.zeros(inside[place].shape, f32)
            body(*inside[:place], *inside[place + 1 :])

        *results, token = pl.pallas_call(
            chained,
            out_shape=[*outs, jax.ShapeDtypeStruct((8, 128), f32)],
            in_specs=[VMEM] * has + list(in_specs),
            out_specs=[*out_specs, VMEM],
            scratch_shapes=list(scratch),
            input_output_aliases={i + has: o for i, o in (aliases or {}).items()},
            cost_estimate=pl.CostEstimate(flops=flops, bytes_accessed=moved, transcendentals=0),
            compiler_params=pltpu.CompilerParams(vmem_limit_bytes=limit_bytes),
        )(*([self.token] * has), *args)
        self.token = token
        return results


def tn(a, b):
    return lax.dot_general(a, b, (((0,), (0,)), ((), ())), preferred_element_type=f32)


def nt(a, b):
    return lax.dot_general(a, b, (((1,), (1,)), ((), ())), preferred_element_type=f32)


def nn(a, b):
    return jnp.dot(a, b, preferred_element_type=f32)


def slot_position(doc_ref, slot):
    first = jnp.int32(0)
    start = jnp.int32(0)
    for j in range(doc_ref.shape[0]):
        start = jnp.where(first <= slot, jnp.maximum(start, first), start)
        first = first + doc_ref[j]
    return slot - start


def fetch(pairs, sems):
    copies = [pltpu.make_async_copy(src, dst, sems.at[i]) for i, (src, dst) in enumerate(pairs)]
    for copy in copies:
        copy.start()
    return copies


def prep_body(work, reach, plan_hbm, doc_hbm, media_ref, *rest):
    sends = rest[:reach]
    own_ref, facts_ref, plan_ref, doc_ref, sems, own_sems, more = rest[reach:]
    slots, tokens, width = media_ref.shape
    early = fetch([(plan_hbm, plan_ref), (doc_hbm, doc_ref)], more)
    for copy in early:
        copy.wait()
    codes = [plan_ref[0, s] for s in range(slots)]
    chosen = []
    for k in range(1, reach + 1):
        slot = jnp.int32(0)
        mark = jnp.int32(0)
        for s in range(slots):
            hit = (codes[s] >= k * work) & (codes[s] < (k + 1) * work)
            slot = jnp.where(hit, s, slot)
            mark = jnp.where(hit, codes[s] - k * work + 1, mark)
        chosen.append((slot, mark))
    copies = fetch(
        [(media_ref.at[slot], sends[k].at[pl.ds(0, tokens)]) for k, (slot, _) in enumerate(chosen)],
        sems,
    )
    own_slots = [jnp.int32(0)] * work
    own_codes = [jnp.int32(0)] * work
    rank = jnp.int32(0)
    for s in range(slots):
        own = (codes[s] >= 0) & (codes[s] < work)
        for w in range(work):
            hit = own & (rank == w)
            own_slots[w] = jnp.where(hit, s, own_slots[w])
            own_codes[w] = jnp.where(hit, codes[s], own_codes[w])
        rank = rank + own.astype(jnp.int32)
    own_copies = fetch([(media_ref.at[own_slots[w]], own_ref.at[w]) for w in range(work)], own_sems)

    def splat(value, height=1):
        return jnp.full((height, width), value.astype(f32), f32)

    facts_ref[...] = jnp.zeros(facts_ref.shape, f32)
    facts_ref[pl.ds(2 * work, 1), :] = splat(rank)
    for w in range(work):
        facts_ref[pl.ds(w, 1), :] = splat(own_codes[w])
        facts_ref[pl.ds(work + w, 1), :] = splat(slot_position(doc_ref, own_slots[w]))
    for k in range(reach):
        slot, mark = chosen[k]
        row = lax.broadcasted_iota(jnp.int32, (MARK_ROWS, width), 0)
        place = splat(slot_position(doc_ref, slot), MARK_ROWS)
        signs = jnp.where(row == 0, splat(mark, MARK_ROWS), place)
        sends[k][pl.ds(tokens, MARK_ROWS), :] = signs.astype(bf16)
    for copy in copies + own_copies:
        copy.wait()


def table_body(time_hbm, out_ref, held, sems):
    (copy,) = fetch([(time_hbm, held)], sems)
    copy.wait()
    out_ref[...] = held[...].astype(f32)


def seen_at(work, reach, place):
    return min(max(reach - work + place + 1, 0), reach)


def select_body(work, reach, place, facts_ref, time_ref, own_ref, *rest):
    seen = seen_at(work, reach, place)
    arrivals = rest[:seen]
    out_ref, info_ref = rest[seen:]
    tokens, width = out_ref.shape
    own_count = facts_ref[pl.ds(2 * work, 1), :]
    signs = [ref[pl.ds(tokens, MARK_ROWS), :].astype(f32) for ref in arrivals]
    marks = [sign[0:1] for sign in signs]
    lives = [jnp.minimum(mark, 1.0) for mark in marks]
    taken = jnp.zeros((1, width), f32)
    for p in range(place + 1):
        ready = own_count
        for live in lives[: seen_at(work, reach, p)]:
            ready = ready + live
        before = taken
        taken = jnp.minimum(taken + 1.0, ready)
    alive = taken - before
    target = jnp.zeros((1, width), f32)
    position = jnp.zeros((1, width), f32)
    raw = jnp.zeros((tokens, width), bf16)
    for w in range(min(work, place + 1)):
        weight = jnp.where((before == w) & (own_count > w), 1.0, 0.0)
        target = target + weight * facts_ref[pl.ds(w, 1), :]
        position = position + weight * facts_ref[pl.ds(work + w, 1), :]
        raw = raw + own_ref[w] * weight.astype(bf16)
    rank = own_count
    for k in range(seen):
        weight = jnp.where(rank == before, lives[k], 0.0)
        target = target + weight * (marks[k] - 1.0)
        position = position + weight * signs[k][1:2]
        raw = raw + arrivals[k][pl.ds(0, tokens), :] * weight.astype(bf16)
        rank = rank + lives[k]
    table = time_ref[...]
    rows = lax.broadcasted_iota(jnp.int32, table.shape, 0).astype(f32)
    row = jnp.sum(jnp.where(rows == position, table, 0.0), axis=0, keepdims=True) * alive
    out_ref[...] = (raw.astype(f32) + row).astype(bf16)
    lanes = info_ref.shape[1]
    info_ref[...] = jnp.zeros(info_ref.shape, f32)
    info_ref[pl.ds(0, 1), :] = target[:, :lanes]
    info_ref[pl.ds(1, 1), :] = alive[:, :lanes]


def normalise(rows):
    average = jnp.mean(rows, axis=-1, keepdims=True)
    centred = rows - average
    spread = jnp.mean(centred * centred, axis=-1, keepdims=True)
    return centred * lax.rsqrt(spread + norm_epsilon)


def own_block(shape, row_size, col_size):
    rows = lax.broadcasted_iota(jnp.int32, shape, 0) // row_size
    cols = lax.broadcasted_iota(jnp.int32, shape, 1) // col_size
    return rows == cols


def spread_heads(rows):
    heads = rows.shape[1] // HEAD
    tall = jnp.concatenate([rows.astype(f32)] * heads, axis=0)
    return jnp.where(own_block(tall.shape, rows.shape[0], HEAD), tall, 0.0)


def assemble(dst, blocks, parts, width):
    me = lax.axis_index("mp")
    for b in range(parts):
        start = pl.multiple_of((me ^ b) * width, width)
        dst[pl.ds(0, blocks[b].shape[0]), pl.ds(start, width)] = blocks[b][...]


def slot_hit(info_ref, slot):
    target = info_ref[pl.ds(0, 1), pl.ds(0, 1)]
    return jnp.where(target == slot, info_ref[pl.ds(1, 1), pl.ds(0, 1)], 0.0)


def place_body(parts, first, last, scale, split, info_ref, *refs):
    blocks, refs = refs[:parts], refs[parts:]
    kw_ref, vw_ref, refs = refs[0], refs[1], refs[2:]
    if first:
        latents_ref, queries_ref, ow_ref, refs = *refs[:3], refs[3:]
        cots, refs = refs[:parts], refs[parts:]
        acc_ref, lat_ref, att_ref, ga_ref, lk_ref, lv_ref, qt_ref, q_ref, norm_ref, *refs = refs
        full, keys, values, grads, cot_full = refs
    else:
        acc_in, lat_in, ga_ref, lk_ref, lv_ref, qt_ref, q_ref, norm_ref, *refs = refs
        if last:
            *done, att_ref, full, keys, values, grads, late = refs
        else:
            acc_ref, lat_ref, att_ref, full, keys, values, grads = refs
    tokens, width = blocks[0].shape
    latents = lk_ref.shape[0]
    inner = kw_ref.shape[1]
    assemble(full, blocks, parts, width)
    chunk = tokens if tokens % 32 else 32
    for r in range(0, tokens, chunk):
        rows = full[pl.ds(r, chunk), :].astype(f32)
        full[pl.ds(r, chunk), :] = normalise(rows).astype(bf16)
    if first:
        assemble(cot_full, cots, parts, width)
        normed = normalise(latents_ref[...].astype(f32)).astype(bf16)
        norm_ref[...] = normed
        full[pl.ds(tokens, latents), :] = normed
        keys[...] = nn(full[...], kw_ref[...]).astype(bf16)
        values[...] = nn(full[...], vw_ref[...]).astype(bf16)
        lk_ref[...] = keys[pl.ds(tokens, latents), :]
        lv_ref[...] = values[pl.ds(tokens, latents), :]
        tall = spread_heads(queries_ref[...])
        q_ref[...] = tall.astype(bf16)
        qt_ref[...] = tall.T.astype(bf16)
        ga_ref[...] = nt(cot_full[...], ow_ref[...]).astype(bf16)
    else:
        keys[pl.ds(0, tokens), :] = nn(full[...], kw_ref[...]).astype(bf16)
        values[pl.ds(0, tokens), :] = nn(full[...], vw_ref[...]).astype(bf16)
        keys[pl.ds(tokens, latents), :] = lk_ref[...]
        values[pl.ds(tokens, latents), :] = lv_ref[...]
    scores = nn(keys[...], qt_ref[...]) * 0.125
    raised = jnp.exp(scores - jnp.max(scores, axis=0, keepdims=True))
    attention = raised / jnp.sum(raised, axis=0, keepdims=True)
    attention_b = attention.astype(bf16)
    crossed = tn(attention_b, values[...])
    crossed = jnp.where(own_block(crossed.shape, latents, HEAD), crossed, 0.0)
    heads = crossed.shape[0] // latents
    att_ref[...] = sum(crossed[h * latents : (h + 1) * latents] for h in range(heads)).astype(bf16)
    ga = jnp.zeros((latents, inner), f32)
    for w in range(ga_ref.shape[0] // latents):
        ga = ga + ga_ref[pl.ds(w * latents, latents), :].astype(f32) * slot_hit(info_ref, w)
    tall = spread_heads(ga)
    grad_weights = nn(values[...], tall.T.astype(bf16))
    row_dot = jnp.sum(attention * grad_weights, axis=0, keepdims=True)
    grad_scores = attention * (grad_weights - row_dot)
    high = grad_scores.astype(bf16)
    low = (grad_scores - high.astype(f32)).astype(bf16)
    grad_keys = ((nn(high, q_ref[...]) + nn(low, q_ref[...])) * 0.125).astype(bf16)
    grad_values = nn(attention_b, tall.astype(bf16)).astype(bf16)
    grads[:, pl.ds(0, inner)] = grad_keys[:tokens]
    grads[:, pl.ds(inner, inner)] = grad_values[:tokens]
    late_rows = [grad_keys[tokens:].astype(f32), grad_values[tokens:].astype(f32)]
    if not first:
        late_rows = [lat_in[:, i * inner : (i + 1) * inner] + late_rows[i] for i in range(2)]
    if not last:
        term = tn(full[pl.ds(0, tokens), :], grads[...])
        acc_ref[...] = term if first else acc_in[...] + term
        lat_ref[:, pl.ds(0, inner)] = late_rows[0]
        lat_ref[:, pl.ds(inner, inner)] = late_rows[1]
        return
    twice = jnp.concatenate([norm_ref[...]] * 2, axis=0)
    for i in range(2):
        columns = slice(i * inner, (i + 1) * inner)
        high = late_rows[i].astype(bf16)
        low = (late_rows[i] - high.astype(f32)).astype(bf16)
        total = tn(full[pl.ds(0, tokens), :], grads[:, columns]) + tn(twice, jnp.concatenate([high, low], axis=0))
        if not first:
            total = total + acc_in[:, columns]
        if split is None:
            done[i][...] = (total * scale).astype(bf16)
            continue
        rows, count, bits = split
        late[...] = total * scale
        bit = bits[i]
        mine = (lax.axis_index("dp") // bit) % 2
        for j in range(count // 2):
            for side in range(2):
                chosen = mine if side == 0 else 1 - mine
                block = (j // bit) * 2 * bit + chosen * bit + j % bit
                at = pl.multiple_of(block * rows, rows)
                done[2 * i + side][pl.ds(j * rows, rows), :] = late[pl.ds(at, rows), :].astype(bf16)


def out_body(work, parts, *refs):
    infos = refs[:work]
    atts = refs[work : 2 * work]
    latents_ref, ow_ref, out_ref, base_ref, rows = refs[2 * work :]
    latents = latents_ref.shape[0]
    width = base_ref.shape[2]
    for p in range(work):
        rows[pl.ds(p * latents, latents), :] = atts[p][...]
    me = lax.axis_index("mp")
    start = pl.multiple_of(me * width, width)
    mine = latents_ref[:, pl.ds(start, width)]
    for j in range(parts):
        part = nn(rows[...], ow_ref[:, j * width : (j + 1) * width])
        for w in range(work):
            value = jnp.zeros((latents, width), f32)
            for p in range(work):
                rows_p = part[p * latents : (p + 1) * latents]
                value = value + rows_p * slot_hit(infos[p], w)
            out_ref[j, pl.ds(w * latents, latents), :] = value.astype(bf16)
    for w in range(work):
        live = jnp.zeros((1, 1), f32)
        for p in range(work):
            live = live + slot_hit(infos[p], w)
        base_ref[w] = mine.astype(f32) * live


def gather_blocks(block, axis):
    size = lax.axis_size(axis)
    blocks = {0: block}
    bit = size // 2
    while bit >= 1:
        for key in list(blocks):
            blocks[key ^ bit] = flip(blocks[key], axis, bit)
        bit //= 2
    return [blocks[b] for b in range(size)]


def pick_side(value, axis, bit_axis, bit):
    mine = (lax.axis_index(axis) // bit) % 2
    keep = lax.dynamic_index_in_dim(value, mine, bit_axis, keepdims=True)
    send = lax.dynamic_index_in_dim(value, 1 - mine, bit_axis, keepdims=True)
    return keep, send


def exchange(keep, send, axis, bit, last):
    got = flip(send, axis, bit)
    total = keep.astype(f32) + got.astype(f32)
    return total if last else total.astype(bf16)


def powers(size):
    found = []
    while 2 ** len(found) < size:
        found.append(2 ** len(found))
    return found


def layer(
    media,
    time_table,
    doc_images,
    plan,
    latents,
    queries,
    key_weight,
    value_weight,
    out_weight,
    cotangent,
):
    slots, tokens, width = media.shape
    work, latent_count, _ = cotangent.shape
    reach = slots - work
    model_width = latents.shape[1]
    inner = queries.shape[1]
    heads = inner // HEAD
    cross = heads * latent_count
    parts = lax.axis_size("mp")
    dp = lax.axis_size("dp")
    bits = powers(dp)
    depth = len(bits)
    turned = bits[1:] + bits[:1]
    rows = model_width // dp
    shape = jax.ShapeDtypeStruct
    chain = Chain()

    fact_rows = -(-(2 * work + 1) // 8) * 8
    *sends, own, facts = chain.call(
        functools.partial(prep_body, work, reach),
        [shape((tokens + MARK_ROWS, width), bf16)] * reach
        + [shape((work, tokens, width), bf16), shape((fact_rows, width), f32)],
        [HBM] * 3,
        [VMEM] * (reach + 2),
        (plan, doc_images, media),
        [
            pltpu.SMEM(plan.shape, jnp.int32),
            pltpu.SMEM(doc_images.shape, jnp.int32),
            pltpu.SemaphoreType.DMA((reach,)),
            pltpu.SemaphoreType.DMA((work,)),
            pltpu.SemaphoreType.DMA((2,)),
        ],
        moved=(reach + work) * tokens * width * 4,
        full=True,
        spare=SPARE,
    )
    arrivals = []
    for k in range(2, reach + 1):
        arrivals.append(from_behind(sends[k - 1], "dp", k))
    if dp % 2 == 0:
        near = flip(sends[0], "dp", 1)
        route = [(i, i if i % 2 else (i + 2) % dp) for i in range(dp)]
        arrivals.append(lax.ppermute(near, "dp", route))
    else:
        arrivals.append(from_behind(sends[0], "dp", 1))
    cot_blocks = gather_blocks(cotangent.reshape(work * latent_count, width), "mp")
    (table,) = chain.call(
        table_body,
        [shape(time_table.shape, f32)],
        [HBM],
        [VMEM],
        (time_table,),
        [pltpu.VMEM(time_table.shape, bf16), pltpu.SemaphoreType.DMA((1,))],
        limit=1,
    )
    infos = []
    gathered = []
    attended = []
    sums = ()
    shared = ()

    def select(p):
        seen = seen_at(work, reach, p)
        block, info = chain.call(
            functools.partial(select_body, work, reach, p),
            [shape((tokens, width), bf16), shape((8, 128), f32)],
            [VMEM] * (seen + 3),
            [VMEM, VMEM],
            (facts, table, own, *arrivals[:seen]),
            moved=tokens * width * 4,
            limit=2,
        )
        infos.append(info)
        gathered.append(gather_blocks(block, "mp"))

    def place(p):
        nonlocal sums, shared
        first, last = p == 0, p == work - 1
        held_rows = tokens + latent_count
        split = None
        new = [
            shape((model_width, 2 * inner), f32),
            shape((latent_count, 2 * inner), f32),
        ]
        if last:
            if rows % 16 == 0 and depth:
                split = (rows, dp, (bits[0], turned[0]))
                new = [shape((model_width // 2, inner), bf16)] * 4
            else:
                new = [shape((model_width, inner), bf16)] * 2
        scratch = [
            pltpu.VMEM((held_rows if first else tokens, model_width), bf16),
            pltpu.VMEM((held_rows, inner), bf16),
            pltpu.VMEM((held_rows, inner), bf16),
            pltpu.VMEM((tokens, 2 * inner), bf16),
        ]
        args = (infos[p], *gathered[p], key_weight, value_weight)
        extra = []
        if first:
            args += (latents, queries, out_weight, *cot_blocks)
            extra = [
                shape((work * latent_count, inner), bf16),
                shape((latent_count, inner), bf16),
                shape((latent_count, inner), bf16),
                shape((inner, cross), bf16),
                shape((cross, inner), bf16),
                shape((latent_count, model_width), bf16),
            ]
            scratch.append(pltpu.VMEM((work * latent_count, model_width), bf16))
        else:
            args += (*sums, *shared)
        if last:
            scratch.append(pltpu.VMEM((model_width, inner), f32))
        start = 3 + parts
        results = chain.call(
            functools.partial(place_body, parts, first, last, 1.0 / (dp * work), split),
            [*new, shape((latent_count, inner), bf16), *extra],
            [VMEM] * len(args),
            [VMEM] * (len(new) + 1 + len(extra)),
            args,
            scratch,
            flops=8 * tokens * model_width * inner + 14 * held_rows * inner * cross,
            limit=16,
            aliases={} if first or last else {start: 0, start + 1: 1},
        )
        sums = tuple(results[: len(new)])
        attended.append(results[len(new)])
        if first:
            shared = tuple(results[len(new) + 1 :])

    for p in range(work):
        if p == 2:
            place(0)
        select(p)
    for p in range(int(work > 2), work):
        place(p)
    carried = sums

    grads = []
    for i, order in enumerate((bits, turned)):
        left = list(reversed(bits))
        if len(carried) == 4:
            keep, send = carried[2 * i : 2 * i + 2]
            left.remove(order[0])
            dims = (2,) * len(left) + (rows, inner)
            part = exchange(keep, send, "dp", order[0], depth == 1).reshape(dims)
            order = order[1:]
        else:
            part = carried[i].reshape((2,) * depth + (rows, inner))
        grads.append([part, left, order])
    for step in range(max((len(g[2]) for g in grads), default=0)):
        for g in grads:
            part, left, order = g
            bit = order[step]
            keep, send = pick_side(part, "dp", left.index(bit), bit)
            part = exchange(keep, send, "dp", bit, step == len(order) - 1)
            left.remove(bit)
            g[0] = part.reshape((2,) * len(left) + (rows, inner))
    key_grad, value_grad = [g[0].astype(f32) for g in grads]

    partial_out, base = chain.call(
        functools.partial(out_body, work, parts),
        [
            shape((parts, work * latent_count, width), bf16),
            shape((work, latent_count, width), f32),
        ],
        [VMEM] * (2 * work + 2),
        [VMEM] * 2,
        (*infos, *attended, latents, out_weight),
        [pltpu.VMEM((work * latent_count, inner), bf16)],
        flops=2 * work * latent_count * inner * model_width,
        limit=8,
    )
    out_bits = powers(parts)
    out = partial_out.reshape((2,) * len(out_bits) + partial_out.shape[1:])
    for step, bit in enumerate(out_bits):
        keep, send = pick_side(out, "mp", len(out_bits) - 1 - step, bit)
        out = exchange(keep, send, "mp", bit, step == len(out_bits) - 1)
    resampled = (base + out.reshape(base.shape)).astype(bf16)
    return (resampled, key_grad, value_grad)


def solution(mesh):
    return jax.shard_map(
        layer,
        mesh=mesh,
        in_specs=(
            P("dp", None, "mp"),
            P(None, "mp"),
            P("dp"),
            P("dp", None),
            P(),
            P(None, "mp"),
            P(None, "mp"),
            P(None, "mp"),
            P("mp", None),
            P("dp", None, "mp"),
        ),
        out_specs=(P("dp", None, "mp"), P("dp", "mp"), P("dp", "mp")),
        check_vma=False,
    )
```

```python
import functools

import jax
import jax.numpy as jnp
from jax import lax
from jax.experimental import pallas as pl
from jax.experimental.pallas import tpu as pltpu
from jax.sharding import PartitionSpec as P


HEAD = 64
MARK_ROWS = 8
VMEM_BYTES = 67043328
SPARE = 12000000
norm_epsilon = 1e-05
f32 = jnp.float32
bf16 = jnp.bfloat16
VMEM = pl.BlockSpec(memory_space=pltpu.VMEM)
HBM = pl.BlockSpec(memory_space=pltpu.HBM)


def from_behind(block, axis, distance):
    size = lax.axis_size(axis)
    route = [(i, (i + distance) % size) for i in range(size)]
    if distance >= 3:
        route = [(i, j) for i, j in route if j > i]
    return lax.ppermute(block, axis, route)


def flip(block, axis, bit):
    return lax.ppermute(block, axis, [(i, i ^ bit) for i in range(lax.axis_size(axis))])


class Chain:
    def __init__(self):
        self.token = None

    def call(
        self,
        body,
        outs,
        in_specs,
        out_specs,
        args,
        scratch=(),
        flops=0,
        moved=0,
        limit=8,
        aliases=None,
        full=False,
        spare=0,
    ):
        has = self.token is not None
        limit_bytes = limit << 20
        if full:
            held = sum(
                o.size * o.dtype.itemsize
                for o, spec in zip(outs, out_specs)
                if spec.memory_space == pltpu.VMEM
            )
            limit_bytes = VMEM_BYTES - held - spare

        def chained(*refs):
            inside = refs[has:]
            place = len(args) + len(outs)
            inside[place][...] = jnp.zeros(inside[place].shape, f32)
            body(*inside[:place], *inside[place + 1 :])

        *results, token = pl.pallas_call(
            chained,
            out_shape=[*outs, jax.ShapeDtypeStruct((8, 128), f32)],
            in_specs=[VMEM] * has + list(in_specs),
            out_specs=[*out_specs, VMEM],
            scratch_shapes=list(scratch),
            input_output_aliases={i + has: o for i, o in (aliases or {}).items()},
            cost_estimate=pl.CostEstimate(flops=flops, bytes_accessed=moved, transcendentals=0),
            compiler_params=pltpu.CompilerParams(vmem_limit_bytes=limit_bytes),
        )(*([self.token] * has), *args)
        self.token = token
        return results


def tn(a, b):
    return lax.dot_general(a, b, (((0,), (0,)), ((), ())), preferred_element_type=f32)


def nt(a, b):
    return lax.dot_general(a, b, (((1,), (1,)), ((), ())), preferred_element_type=f32)


def nn(a, b):
    return jnp.dot(a, b, preferred_element_type=f32)


def slot_position(doc_ref, slot):
    first = jnp.int32(0)
    start = jnp.int32(0)
    for j in range(doc_ref.shape[0]):
        start = jnp.where(first <= slot, jnp.maximum(start, first), start)
        first = first + doc_ref[j]
    return slot - start


def fetch(pairs, sems):
    copies = [pltpu.make_async_copy(src, dst, sems.at[i]) for i, (src, dst) in enumerate(pairs)]
    for copy in copies:
        copy.start()
    return copies


def prep_body(work, reach, plan_hbm, doc_hbm, media_ref, *rest):
    sends = rest[:reach]
    own_ref, facts_ref, plan_ref, doc_ref, sems, own_sems, more = rest[reach:]
    slots, tokens, width = media_ref.shape
    early = fetch([(plan_hbm, plan_ref), (doc_hbm, doc_ref)], more)
    for copy in early:
        copy.wait()
    codes = [plan_ref[0, s] for s in range(slots)]
    chosen = []
    for k in range(1, reach + 1):
        slot = jnp.int32(0)
        mark = jnp.int32(0)
        for s in range(slots):
            hit = (codes[s] >= k * work) & (codes[s] < (k + 1) * work)
            slot = jnp.where(hit, s, slot)
            mark = jnp.where(hit, codes[s] - k * work + 1, mark)
        chosen.append((slot, mark))
    copies = fetch(
        [(media_ref.at[slot], sends[k].at[pl.ds(0, tokens)]) for k, (slot, _) in enumerate(chosen)],
        sems,
    )
    own_slots = [jnp.int32(0)] * work
    own_codes = [jnp.int32(0)] * work
    rank = jnp.int32(0)
    for s in range(slots):
        own = (codes[s] >= 0) & (codes[s] < work)
        for w in range(work):
            hit = own & (rank == w)
            own_slots[w] = jnp.where(hit, s, own_slots[w])
            own_codes[w] = jnp.where(hit, codes[s], own_codes[w])
        rank = rank + own.astype(jnp.int32)
    own_copies = fetch([(media_ref.at[own_slots[w]], own_ref.at[w]) for w in range(work)], own_sems)

    def splat(value, height=1):
        return jnp.full((height, width), value.astype(f32), f32)

    facts_ref[...] = jnp.zeros(facts_ref.shape, f32)
    facts_ref[pl.ds(2 * work, 1), :] = splat(rank)
    for w in range(work):
        facts_ref[pl.ds(w, 1), :] = splat(own_codes[w])
        facts_ref[pl.ds(work + w, 1), :] = splat(slot_position(doc_ref, own_slots[w]))
    for k in range(reach):
        slot, mark = chosen[k]
        row = lax.broadcasted_iota(jnp.int32, (MARK_ROWS, width), 0)
        place = splat(slot_position(doc_ref, slot), MARK_ROWS)
        signs = jnp.where(row == 0, splat(mark, MARK_ROWS), place)
        sends[k][pl.ds(tokens, MARK_ROWS), :] = signs.astype(bf16)
    for copy in copies + own_copies:
        copy.wait()


def table_body(time_hbm, out_ref, held, sems):
    (copy,) = fetch([(time_hbm, held)], sems)
    copy.wait()
    out_ref[...] = held[...].astype(f32)


def seen_at(work, reach, place):
    return min(max(reach - work + place + 1, 0), reach)


def select_body(work, reach, place, facts_ref, time_ref, own_ref, *rest):
    seen = seen_at(work, reach, place)
    arrivals = rest[:seen]
    out_ref, info_ref = rest[seen:]
    tokens, width = out_ref.shape
    own_count = facts_ref[pl.ds(2 * work, 1), :]
    signs = [ref[pl.ds(tokens, MARK_ROWS), :].astype(f32) for ref in arrivals]
    marks = [sign[0:1] for sign in signs]
    lives = [jnp.minimum(mark, 1.0) for mark in marks]
    taken = jnp.zeros((1, width), f32)
    for p in range(place + 1):
        ready = own_count
        for live in lives[: seen_at(work, reach, p)]:
            ready = ready + live
        before = taken
        taken = jnp.minimum(taken + 1.0, ready)
    alive = taken - before
    target = jnp.zeros((1, width), f32)
    position = jnp.zeros((1, width), f32)
    raw = jnp.zeros((tokens, width), bf16)
    for w in range(min(work, place + 1)):
        weight = jnp.where((before == w) & (own_count > w), 1.0, 0.0)
        target = target + weight * facts_ref[pl.ds(w, 1), :]
        position = position + weight * facts_ref[pl.ds(work + w, 1), :]
        raw = raw + own_ref[w] * weight.astype(bf16)
    rank = own_count
    for k in range(seen):
        weight = jnp.where(rank == before, lives[k], 0.0)
        target = target + weight * (marks[k] - 1.0)
        position = position + weight * signs[k][1:2]
        raw = raw + arrivals[k][pl.ds(0, tokens), :] * weight.astype(bf16)
        rank = rank + lives[k]
    table = time_ref[...]
    rows = lax.broadcasted_iota(jnp.int32, table.shape, 0).astype(f32)
    row = jnp.sum(jnp.where(rows == position, table, 0.0), axis=0, keepdims=True) * alive
    out_ref[...] = (raw.astype(f32) + row).astype(bf16)
    lanes = info_ref.shape[1]
    info_ref[...] = jnp.zeros(info_ref.shape, f32)
    info_ref[pl.ds(0, 1), :] = target[:, :lanes]
    info_ref[pl.ds(1, 1), :] = alive[:, :lanes]


def normalise(rows):
    average = jnp.mean(rows, axis=-1, keepdims=True)
    centred = rows - average
    spread = jnp.mean(centred * centred, axis=-1, keepdims=True)
    return centred * lax.rsqrt(spread + norm_epsilon)


def own_block(shape, row_size, col_size):
    rows = lax.broadcasted_iota(jnp.int32, shape, 0) // row_size
    cols = lax.broadcasted_iota(jnp.int32, shape, 1) // col_size
    return rows == cols


def spread_heads(rows):
    heads = rows.shape[1] // HEAD
    tall = jnp.concatenate([rows.astype(f32)] * heads, axis=0)
    return jnp.where(own_block(tall.shape, rows.shape[0], HEAD), tall, 0.0)


def assemble(dst, blocks, parts, width):
    me = lax.axis_index("mp")
    for b in range(parts):
        start = pl.multiple_of((me ^ b) * width, width)
        dst[pl.ds(0, blocks[b].shape[0]), pl.ds(start, width)] = blocks[b][...]


def slot_hit(info_ref, slot):
    target = info_ref[pl.ds(0, 1), pl.ds(0, 1)]
    return jnp.where(target == slot, info_ref[pl.ds(1, 1), pl.ds(0, 1)], 0.0)


def place_body(parts, first, last, scale, split, info_ref, *refs):
    blocks, refs = refs[:parts], refs[parts:]
    kw_ref, vw_ref, refs = refs[0], refs[1], refs[2:]
    if first:
        latents_ref, queries_ref, ow_ref, refs = *refs[:3], refs[3:]
        cots, refs = refs[:parts], refs[parts:]
        acc_ref, lat_ref, att_ref, ga_ref, lk_ref, lv_ref, qt_ref, q_ref, norm_ref, *refs = refs
        full, keys, values, grads, cot_full = refs
    else:
        acc_in, lat_in, ga_ref, lk_ref, lv_ref, qt_ref, q_ref, norm_ref, *refs = refs
        if last:
            *done, att_ref, full, keys, values, grads, late = refs
        else:
            acc_ref, lat_ref, att_ref, full, keys, values, grads = refs
    tokens, width = blocks[0].shape
    latents = lk_ref.shape[0]
    inner = kw_ref.shape[1]
    assemble(full, blocks, parts, width)
    chunk = tokens if tokens % 32 else 32
    for r in range(0, tokens, chunk):
        rows = full[pl.ds(r, chunk), :].astype(f32)
        full[pl.ds(r, chunk), :] = normalise(rows).astype(bf16)
    if first:
        assemble(cot_full, cots, parts, width)
        normed = normalise(latents_ref[...].astype(f32)).astype(bf16)
        norm_ref[...] = normed
        full[pl.ds(tokens, latents), :] = normed
        keys[...] = nn(full[...], kw_ref[...]).astype(bf16)
        values[...] = nn(full[...], vw_ref[...]).astype(bf16)
        lk_ref[...] = keys[pl.ds(tokens, latents), :]
        lv_ref[...] = values[pl.ds(tokens, latents), :]
        tall = spread_heads(queries_ref[...])
        q_ref[...] = tall.astype(bf16)
        qt_ref[...] = tall.T.astype(bf16)
        ga_ref[...] = nt(cot_full[...], ow_ref[...]).astype(bf16)
    else:
        keys[pl.ds(0, tokens), :] = nn(full[...], kw_ref[...]).astype(bf16)
        values[pl.ds(0, tokens), :] = nn(full[...], vw_ref[...]).astype(bf16)
        keys[pl.ds(tokens, latents), :] = lk_ref[...]
        values[pl.ds(tokens, latents), :] = lv_ref[...]
    scores = nn(keys[...], qt_ref[...]) * 0.125
    raised = jnp.exp(scores - jnp.max(scores, axis=0, keepdims=True))
    attention = raised / jnp.sum(raised, axis=0, keepdims=True)
    attention_b = attention.astype(bf16)
    crossed = tn(attention_b, values[...])
    crossed = jnp.where(own_block(crossed.shape, latents, HEAD), crossed, 0.0)
    heads = crossed.shape[0] // latents
    att_ref[...] = sum(crossed[h * latents : (h + 1) * latents] for h in range(heads)).astype(bf16)
    ga = jnp.zeros((latents, inner), f32)
    for w in range(ga_ref.shape[0] // latents):
        ga = ga + ga_ref[pl.ds(w * latents, latents), :].astype(f32) * slot_hit(info_ref, w)
    tall = spread_heads(ga)
    grad_weights = nn(values[...], tall.T.astype(bf16))
    row_dot = jnp.sum(attention * grad_weights, axis=0, keepdims=True)
    grad_scores = attention * (grad_weights - row_dot)
    high = grad_scores.astype(bf16)
    low = (grad_scores - high.astype(f32)).astype(bf16)
    grad_keys = ((nn(high, q_ref[...]) + nn(low, q_ref[...])) * 0.125).astype(bf16)
    grad_values = nn(attention_b, tall.astype(bf16)).astype(bf16)
    grads[:, pl.ds(0, inner)] = grad_keys[:tokens]
    grads[:, pl.ds(inner, inner)] = grad_values[:tokens]
    late_rows = [grad_keys[tokens:].astype(f32), grad_values[tokens:].astype(f32)]
    if not first:
        late_rows = [lat_in[:, i * inner : (i + 1) * inner] + late_rows[i] for i in range(2)]
    if not last:
        term = tn(full[pl.ds(0, tokens), :], grads[...])
        acc_ref[...] = term if first else acc_in[...] + term
        lat_ref[:, pl.ds(0, inner)] = late_rows[0]
        lat_ref[:, pl.ds(inner, inner)] = late_rows[1]
        return
    twice = jnp.concatenate([norm_ref[...]] * 2, axis=0)
    for i in range(2):
        columns = slice(i * inner, (i + 1) * inner)
        high = late_rows[i].astype(bf16)
        low = (late_rows[i] - high.astype(f32)).astype(bf16)
        total = tn(full[pl.ds(0, tokens), :], grads[:, columns]) + tn(twice, jnp.concatenate([high, low], axis=0))
        if not first:
            total = total + acc_in[:, columns]
        if split is None:
            done[i][...] = (total * scale).astype(bf16)
            continue
        rows, count, bits = split
        late[...] = total * scale
        bit = bits[i]
        mine = (lax.axis_index("dp") // bit) % 2
        for j in range(count // 2):
            for side in range(2):
                chosen = mine if side == 0 else 1 - mine
                block = (j // bit) * 2 * bit + chosen * bit + j % bit
                at = pl.multiple_of(block * rows, rows)
                done[2 * i + side][pl.ds(j * rows, rows), :] = late[pl.ds(at, rows), :].astype(bf16)


def out_body(work, parts, *refs):
    infos = refs[:work]
    atts = refs[work : 2 * work]
    latents_ref, ow_ref, out_ref, base_ref, rows = refs[2 * work :]
    latents = latents_ref.shape[0]
    width = base_ref.shape[2]
    for p in range(work):
        rows[pl.ds(p * latents, latents), :] = atts[p][...]
    me = lax.axis_index("mp")
    start = pl.multiple_of(me * width, width)
    mine = latents_ref[:, pl.ds(start, width)]
    for j in range(parts):
        part = nn(rows[...], ow_ref[:, j * width : (j + 1) * width])
        for w in range(work):
            value = jnp.zeros((latents, width), f32)
            for p in range(work):
                rows_p = part[p * latents : (p + 1) * latents]
                value = value + rows_p * slot_hit(infos[p], w)
            out_ref[j, pl.ds(w * latents, latents), :] = value.astype(bf16)
    for w in range(work):
        live = jnp.zeros((1, 1), f32)
        for p in range(work):
            live = live + slot_hit(infos[p], w)
        base_ref[w] = mine.astype(f32) * live


def gather_blocks(block, axis):
    size = lax.axis_size(axis)
    blocks = {0: block}
    bit = size // 2
    while bit >= 1:
        for key in list(blocks):
            blocks[key ^ bit] = flip(blocks[key], axis, bit)
        bit //= 2
    return [blocks[b] for b in range(size)]


def pick_side(value, axis, bit_axis, bit):
    mine = (lax.axis_index(axis) // bit) % 2
    keep = lax.dynamic_index_in_dim(value, mine, bit_axis, keepdims=True)
    send = lax.dynamic_index_in_dim(value, 1 - mine, bit_axis, keepdims=True)
    return keep, send


def exchange(keep, send, axis, bit, last):
    got = flip(send, axis, bit)
    total = keep.astype(f32) + got.astype(f32)
    return total if last else total.astype(bf16)


def fold_body(rows, bit, *refs):
    send_ref, keep_ref = refs[4:]
    mine = (lax.axis_index("dp") // bit) % 2
    ours = pl.ds(pl.multiple_of(mine * rows, rows), rows)
    theirs = pl.ds(pl.multiple_of((1 - mine) * rows, rows), rows)
    for i in range(2):
        held, got = refs[2 * i], refs[2 * i + 1]
        out = pl.ds(i * rows, rows)
        keep_ref[out, :] = held[ours, :].astype(f32) + got[ours, :].astype(f32)
        total = held[theirs, :].astype(f32) + got[theirs, :].astype(f32)
        send_ref[out, :] = total.astype(bf16)


def finish_body(keep_ref, got_ref, key_ref, value_ref):
    rows = key_ref.shape[0]
    for i, out in enumerate((key_ref, value_ref)):
        part = pl.ds(i * rows, rows)
        out[...] = keep_ref[part, :] + got_ref[part, :].astype(f32)


def merged_exchange(keeps, sends, rows, inner, bits):
    low, middle, high = bits
    shape = jax.ShapeDtypeStruct
    sides = []
    for keep, send, first, second in (
        (keeps[0], sends[0], low, middle),
        (keeps[1], sends[1], middle, low),
    ):
        part = exchange(keep, send, "dp", first, False).reshape(2, 2, rows, inner)
        keep, send = pick_side(part, "dp", 1, second)
        got = flip(send.reshape(2 * rows, inner), "dp", second)
        sides += [keep.reshape(2 * rows, inner), got]
    send, keep = Chain().call(
        functools.partial(fold_body, rows, high),
        [shape((2 * rows, inner), bf16), shape((2 * rows, inner), f32)],
        [VMEM] * 4,
        [VMEM] * 2,
        sides,
        moved=16 * rows * inner,
        limit=4,
    )
    return Chain().call(
        finish_body,
        [shape((rows, inner), f32)] * 2,
        [VMEM] * 2,
        [VMEM] * 2,
        (keep, flip(send, "dp", high)),
        moved=16 * rows * inner,
        limit=4,
    )


def powers(size):
    found = []
    while 2 ** len(found) < size:
        found.append(2 ** len(found))
    return found


def layer(
    media,
    time_table,
    doc_images,
    plan,
    latents,
    queries,
    key_weight,
    value_weight,
    out_weight,
    cotangent,
):
    slots, tokens, width = media.shape
    work, latent_count, _ = cotangent.shape
    reach = slots - work
    model_width = latents.shape[1]
    inner = queries.shape[1]
    heads = inner // HEAD
    cross = heads * latent_count
    parts = lax.axis_size("mp")
    dp = lax.axis_size("dp")
    bits = powers(dp)
    depth = len(bits)
    turned = bits[1:2] + bits[:1] + bits[2:]
    rows = model_width // dp
    shape = jax.ShapeDtypeStruct
    chain = Chain()

    fact_rows = -(-(2 * work + 1) // 8) * 8
    *sends, own, facts = chain.call(
        functools.partial(prep_body, work, reach),
        [shape((tokens + MARK_ROWS, width), bf16)] * reach
        + [shape((work, tokens, width), bf16), shape((fact_rows, width), f32)],
        [HBM] * 3,
        [VMEM] * (reach + 2),
        (plan, doc_images, media),
        [
            pltpu.SMEM(plan.shape, jnp.int32),
            pltpu.SMEM(doc_images.shape, jnp.int32),
            pltpu.SemaphoreType.DMA((reach,)),
            pltpu.SemaphoreType.DMA((work,)),
            pltpu.SemaphoreType.DMA((2,)),
        ],
        moved=(reach + work) * tokens * width * 4,
        full=True,
        spare=SPARE,
    )
    arrivals = []
    for k in range(2, reach + 1):
        arrivals.append(from_behind(sends[k - 1], "dp", k))
    if dp % 2 == 0:
        near = flip(sends[0], "dp", 1)
        route = [(i, i if i % 2 else (i + 2) % dp) for i in range(dp)]
        arrivals.append(lax.ppermute(near, "dp", route))
    else:
        arrivals.append(from_behind(sends[0], "dp", 1))
    cot_blocks = gather_blocks(cotangent.reshape(work * latent_count, width), "mp")
    (table,) = chain.call(
        table_body,
        [shape(time_table.shape, f32)],
        [HBM],
        [VMEM],
        (time_table,),
        [pltpu.VMEM(time_table.shape, bf16), pltpu.SemaphoreType.DMA((1,))],
        limit=1,
    )
    infos = []
    gathered = []
    attended = []
    sums = ()
    shared = ()

    def select(p):
        seen = seen_at(work, reach, p)
        block, info = chain.call(
            functools.partial(select_body, work, reach, p),
            [shape((tokens, width), bf16), shape((8, 128), f32)],
            [VMEM] * (seen + 3),
            [VMEM, VMEM],
            (facts, table, own, *arrivals[:seen]),
            moved=tokens * width * 4,
            limit=2,
        )
        infos.append(info)
        gathered.append(gather_blocks(block, "mp"))

    def place(p):
        nonlocal sums, shared
        first, last = p == 0, p == work - 1
        held_rows = tokens + latent_count
        split = None
        new = [
            shape((model_width, 2 * inner), f32),
            shape((latent_count, 2 * inner), f32),
        ]
        if last:
            if rows % 16 == 0 and depth:
                split = (rows, dp, (bits[0], turned[0]))
                new = [shape((model_width // 2, inner), bf16)] * 4
            else:
                new = [shape((model_width, inner), bf16)] * 2
        scratch = [
            pltpu.VMEM((held_rows if first else tokens, model_width), bf16),
            pltpu.VMEM((held_rows, inner), bf16),
            pltpu.VMEM((held_rows, inner), bf16),
            pltpu.VMEM((tokens, 2 * inner), bf16),
        ]
        args = (infos[p], *gathered[p], key_weight, value_weight)
        extra = []
        if first:
            args += (latents, queries, out_weight, *cot_blocks)
            extra = [
                shape((work * latent_count, inner), bf16),
                shape((latent_count, inner), bf16),
                shape((latent_count, inner), bf16),
                shape((inner, cross), bf16),
                shape((cross, inner), bf16),
                shape((latent_count, model_width), bf16),
            ]
            scratch.append(pltpu.VMEM((work * latent_count, model_width), bf16))
        else:
            args += (*sums, *shared)
        if last:
            scratch.append(pltpu.VMEM((model_width, inner), f32))
        start = 3 + parts
        results = chain.call(
            functools.partial(place_body, parts, first, last, 1.0 / (dp * work), split),
            [*new, shape((latent_count, inner), bf16), *extra],
            [VMEM] * len(args),
            [VMEM] * (len(new) + 1 + len(extra)),
            args,
            scratch,
            flops=8 * tokens * model_width * inner + 14 * held_rows * inner * cross,
            limit=16,
            aliases={} if first or last else {start: 0, start + 1: 1},
        )
        sums = tuple(results[: len(new)])
        attended.append(results[len(new)])
        if first:
            shared = tuple(results[len(new) + 1 :])

    for p in range(work):
        if p == 2:
            place(0)
        select(p)
    for p in range(int(work > 2), work):
        place(p)
    carried = sums

    if depth == 3 and len(carried) == 4:
        key_grad, value_grad = merged_exchange(carried[0::2], carried[1::2], rows, inner, bits)
    else:
        grads = []
        for i, order in enumerate((bits, turned)):
            left = list(reversed(bits))
            if len(carried) == 4:
                keep, send = carried[2 * i : 2 * i + 2]
                left.remove(order[0])
                dims = (2,) * len(left) + (rows, inner)
                part = exchange(keep, send, "dp", order[0], depth == 1).reshape(dims)
                order = order[1:]
            else:
                part = carried[i].reshape((2,) * depth + (rows, inner))
            grads.append([part, left, order])
        for step in range(max((len(g[2]) for g in grads), default=0)):
            for g in grads:
                part, left, order = g
                bit = order[step]
                keep, send = pick_side(part, "dp", left.index(bit), bit)
                part = exchange(keep, send, "dp", bit, step == len(order) - 1)
                left.remove(bit)
                g[0] = part.reshape((2,) * len(left) + (rows, inner))
        key_grad, value_grad = [g[0].astype(f32) for g in grads]

    partial_out, base = chain.call(
        functools.partial(out_body, work, parts),
        [
            shape((parts, work * latent_count, width), bf16),
            shape((work, latent_count, width), f32),
        ],
        [VMEM] * (2 * work + 2),
        [VMEM] * 2,
        (*infos, *attended, latents, out_weight),
        [pltpu.VMEM((work * latent_count, inner), bf16)],
        flops=2 * work * latent_count * inner * model_width,
        limit=8,
    )
    out_bits = powers(parts)
    out = partial_out.reshape((2,) * len(out_bits) + partial_out.shape[1:])
    for step, bit in enumerate(out_bits):
        keep, send = pick_side(out, "mp", len(out_bits) - 1 - step, bit)
        out = exchange(keep, send, "mp", bit, step == len(out_bits) - 1)
    resampled = (base + out.reshape(base.shape)).astype(bf16)
    return (resampled, key_grad, value_grad)


def solution(mesh):
    return jax.shard_map(
        layer,
        mesh=mesh,
        in_specs=(
            P("dp", None, "mp"),
            P(None, "mp"),
            P("dp"),
            P("dp", None),
            P(),
            P(None, "mp"),
            P(None, "mp"),
            P(None, "mp"),
            P("mp", None),
            P("dp", None, "mp"),
        ),
        out_specs=(P("dp", None, "mp"), P("dp", "mp"), P("dp", "mp")),
        check_vma=False,
    )
```

```python
import functools

import jax
import jax.numpy as jnp
from jax import lax
from jax.experimental import pallas as pl
from jax.experimental.pallas import tpu as pltpu
from jax.sharding import PartitionSpec as P


HEAD = 64
MARK_ROWS = 8
VMEM_BYTES = 67043328
SPARE = 12000000
norm_epsilon = 1e-05
f32 = jnp.float32
bf16 = jnp.bfloat16
VMEM = pl.BlockSpec(memory_space=pltpu.VMEM)
HBM = pl.BlockSpec(memory_space=pltpu.HBM)


def from_behind(block, axis, distance):
    size = lax.axis_size(axis)
    route = [(i, (i + distance) % size) for i in range(size)]
    if distance >= 3:
        route = [(i, j) for i, j in route if j > i]
    return lax.ppermute(block, axis, route)


def flip(block, axis, bit):
    return lax.ppermute(block, axis, [(i, i ^ bit) for i in range(lax.axis_size(axis))])


class Chain:
    def __init__(self):
        self.token = None

    def call(
        self,
        body,
        outs,
        in_specs,
        out_specs,
        args,
        scratch=(),
        flops=0,
        moved=0,
        limit=8,
        aliases=None,
        alone=False,
        full=False,
        spare=0,
    ):
        has = self.token is not None
        limit_bytes = limit << 20
        if full:
            held = sum(
                o.size * o.dtype.itemsize
                for o, spec in zip(outs, out_specs)
                if spec.memory_space == pltpu.VMEM
            )
            limit_bytes = VMEM_BYTES - held - spare

        def chained(*refs):
            inside = refs[has:]
            place = len(args) + len(outs)
            inside[place][...] = jnp.zeros(inside[place].shape, f32)
            body(*inside[:place], *inside[place + 1 :])

        marks = [] if alone else [jax.ShapeDtypeStruct((8, 128), f32)]
        results = pl.pallas_call(
            body if alone else chained,
            out_shape=[*outs, *marks],
            in_specs=[VMEM] * has + list(in_specs),
            out_specs=[*out_specs, *[VMEM] * len(marks)],
            scratch_shapes=list(scratch),
            input_output_aliases={i + has: o for i, o in (aliases or {}).items()},
            cost_estimate=pl.CostEstimate(flops=flops, bytes_accessed=moved, transcendentals=0),
            compiler_params=pltpu.CompilerParams(vmem_limit_bytes=limit_bytes),
        )(*([self.token] * has), *args)
        if alone:
            return results
        *results, self.token = results
        return results


def tn(a, b):
    return lax.dot_general(a, b, (((0,), (0,)), ((), ())), preferred_element_type=f32)


def nt(a, b):
    return lax.dot_general(a, b, (((1,), (1,)), ((), ())), preferred_element_type=f32)


def nn(a, b):
    return jnp.dot(a, b, preferred_element_type=f32)


def slot_position(counts, slot):
    first = jnp.int32(0)
    start = jnp.int32(0)
    for count in counts:
        start = jnp.where(first <= slot, jnp.maximum(start, first), start)
        first = first + count
    return slot - start


def fetch(pairs, sems):
    copies = [pltpu.make_async_copy(src, dst, sems.at[i]) for i, (src, dst) in enumerate(pairs)]
    for copy in copies:
        copy.start()
    return copies


def prep_body(work, reach, control_hbm, media_ref, *rest):
    sends = rest[:reach]
    own_ref, facts_ref, control_ref, sems, own_sems, more = rest[reach:]
    slots, tokens, width = media_ref.shape
    (early,) = fetch([(control_hbm, control_ref)], more)
    early.wait()
    codes = [control_ref[s] for s in range(slots)]
    counts = [control_ref[s] for s in range(slots, control_ref.shape[0])]
    chosen = []
    for k in range(1, reach + 1):
        slot = jnp.int32(0)
        mark = jnp.int32(0)
        for s in range(slots):
            hit = (codes[s] >= k * work) & (codes[s] < (k + 1) * work)
            slot = jnp.where(hit, s, slot)
            mark = jnp.where(hit, codes[s] - k * work + 1, mark)
        chosen.append((slot, mark))
    copies = fetch(
        [(media_ref.at[slot], sends[k].at[pl.ds(0, tokens)]) for k, (slot, _) in enumerate(chosen)],
        sems,
    )
    own_slots = [jnp.int32(0)] * work
    own_codes = [jnp.int32(0)] * work
    rank = jnp.int32(0)
    for s in range(slots):
        own = (codes[s] >= 0) & (codes[s] < work)
        for w in range(work):
            hit = own & (rank == w)
            own_slots[w] = jnp.where(hit, s, own_slots[w])
            own_codes[w] = jnp.where(hit, codes[s], own_codes[w])
        rank = rank + own.astype(jnp.int32)
    own_copies = fetch([(media_ref.at[own_slots[w]], own_ref.at[w]) for w in range(work)], own_sems)

    def splat(value, height=1):
        return jnp.full((height, width), value.astype(f32), f32)

    facts_ref[...] = jnp.zeros(facts_ref.shape, f32)
    facts_ref[pl.ds(2 * work, 1), :] = splat(rank)
    for w in range(work):
        facts_ref[pl.ds(w, 1), :] = splat(own_codes[w])
        facts_ref[pl.ds(work + w, 1), :] = splat(slot_position(counts, own_slots[w]))
    for k in range(reach):
        slot, mark = chosen[k]
        row = lax.broadcasted_iota(jnp.int32, (MARK_ROWS, width), 0)
        place = splat(slot_position(counts, slot), MARK_ROWS)
        signs = jnp.where(row == 0, splat(mark, MARK_ROWS), place)
        sends[k][pl.ds(tokens, MARK_ROWS), :] = signs.astype(bf16)
    for copy in copies + own_copies:
        copy.wait()


def table_body(time_hbm, out_ref, held, sems):
    (copy,) = fetch([(time_hbm, held)], sems)
    copy.wait()
    out_ref[...] = held[...].astype(f32)


def seen_at(work, reach, place):
    return min(max(reach - work + place + 1, 0), reach)


def select_body(work, reach, place, facts_ref, time_ref, own_ref, *rest):
    seen = seen_at(work, reach, place)
    arrivals = rest[:seen]
    out_ref, info_ref = rest[seen:]
    tokens, width = out_ref.shape
    own_count = facts_ref[pl.ds(2 * work, 1), :]
    signs = [ref[pl.ds(tokens, MARK_ROWS), :].astype(f32) for ref in arrivals]
    marks = [sign[0:1] for sign in signs]
    lives = [jnp.minimum(mark, 1.0) for mark in marks]
    taken = jnp.zeros((1, width), f32)
    for p in range(place + 1):
        ready = own_count
        for live in lives[: seen_at(work, reach, p)]:
            ready = ready + live
        before = taken
        taken = jnp.minimum(taken + 1.0, ready)
    alive = taken - before
    target = jnp.zeros((1, width), f32)
    position = jnp.zeros((1, width), f32)
    raw = jnp.zeros((tokens, width), bf16)
    for w in range(min(work, place + 1)):
        weight = jnp.where((before == w) & (own_count > w), 1.0, 0.0)
        target = target + weight * facts_ref[pl.ds(w, 1), :]
        position = position + weight * facts_ref[pl.ds(work + w, 1), :]
        raw = raw + own_ref[w] * weight.astype(bf16)
    rank = own_count
    for k in range(seen):
        weight = jnp.where(rank == before, lives[k], 0.0)
        target = target + weight * (marks[k] - 1.0)
        position = position + weight * signs[k][1:2]
        raw = raw + arrivals[k][pl.ds(0, tokens), :] * weight.astype(bf16)
        rank = rank + lives[k]
    table = time_ref[...]
    rows = lax.broadcasted_iota(jnp.int32, table.shape, 0).astype(f32)
    row = jnp.sum(jnp.where(rows == position, table, 0.0), axis=0, keepdims=True) * alive
    out_ref[...] = (raw.astype(f32) + row).astype(bf16)
    lanes = info_ref.shape[1]
    info_ref[...] = jnp.zeros(info_ref.shape, f32)
    info_ref[pl.ds(0, 1), :] = target[:, :lanes]
    info_ref[pl.ds(1, 1), :] = alive[:, :lanes]


def normalise(rows):
    average = jnp.mean(rows, axis=-1, keepdims=True)
    centred = rows - average
    spread = jnp.mean(centred * centred, axis=-1, keepdims=True)
    return centred * lax.rsqrt(spread + norm_epsilon)


def own_block(shape, row_size, col_size):
    rows = lax.broadcasted_iota(jnp.int32, shape, 0) // row_size
    cols = lax.broadcasted_iota(jnp.int32, shape, 1) // col_size
    return rows == cols


def spread_heads(rows):
    heads = rows.shape[1] // HEAD
    tall = jnp.concatenate([rows.astype(f32)] * heads, axis=0)
    return jnp.where(own_block(tall.shape, rows.shape[0], HEAD), tall, 0.0)


def assemble(dst, blocks, parts, width):
    me = lax.axis_index("mp")
    for b in range(parts):
        start = pl.multiple_of((me ^ b) * width, width)
        dst[pl.ds(0, blocks[b].shape[0]), pl.ds(start, width)] = blocks[b][...]


def slot_hit(info_ref, slot):
    target = info_ref[pl.ds(0, 1), pl.ds(0, 1)]
    return jnp.where(target == slot, info_ref[pl.ds(1, 1), pl.ds(0, 1)], 0.0)


def place_body(parts, first, last, scale, split, info_ref, *refs):
    blocks, refs = refs[:parts], refs[parts:]
    kw_ref, vw_ref, refs = refs[0], refs[1], refs[2:]
    if first:
        latents_ref, queries_ref, ow_ref, refs = *refs[:3], refs[3:]
        cots, refs = refs[:parts], refs[parts:]
        acc_ref, lat_ref, att_ref, ga_ref, lk_ref, lv_ref, qt_ref, q_ref, norm_ref, *refs = refs
        full, keys, values, grads, cot_full = refs
    else:
        acc_in, lat_in, ga_ref, lk_ref, lv_ref, qt_ref, q_ref, norm_ref, *refs = refs
        if last:
            *done, att_ref, full, keys, values, grads, late = refs
        else:
            acc_ref, lat_ref, att_ref, full, keys, values, grads = refs
    tokens, width = blocks[0].shape
    latents = lk_ref.shape[0]
    inner = kw_ref.shape[1]
    assemble(full, blocks, parts, width)
    chunk = tokens if tokens % 32 else 32
    for r in range(0, tokens, chunk):
        rows = full[pl.ds(r, chunk), :].astype(f32)
        full[pl.ds(r, chunk), :] = normalise(rows).astype(bf16)
    if first:
        assemble(cot_full, cots, parts, width)
        normed = normalise(latents_ref[...].astype(f32)).astype(bf16)
        norm_ref[...] = normed
        full[pl.ds(tokens, latents), :] = normed
        keys[...] = nn(full[...], kw_ref[...]).astype(bf16)
        values[...] = nn(full[...], vw_ref[...]).astype(bf16)
        lk_ref[...] = keys[pl.ds(tokens, latents), :]
        lv_ref[...] = values[pl.ds(tokens, latents), :]
        tall = spread_heads(queries_ref[...])
        q_ref[...] = tall.astype(bf16)
        qt_ref[...] = tall.T.astype(bf16)
        ga_ref[...] = nt(cot_full[...], ow_ref[...]).astype(bf16)
    else:
        keys[pl.ds(0, tokens), :] = nn(full[...], kw_ref[...]).astype(bf16)
        values[pl.ds(0, tokens), :] = nn(full[...], vw_ref[...]).astype(bf16)
        keys[pl.ds(tokens, latents), :] = lk_ref[...]
        values[pl.ds(tokens, latents), :] = lv_ref[...]
    scores = nn(keys[...], qt_ref[...]) * 0.125
    raised = jnp.exp(scores - jnp.max(scores, axis=0, keepdims=True))
    attention = raised / jnp.sum(raised, axis=0, keepdims=True)
    attention_b = attention.astype(bf16)
    crossed = tn(attention_b, values[...])
    crossed = jnp.where(own_block(crossed.shape, latents, HEAD), crossed, 0.0)
    heads = crossed.shape[0] // latents
    att_ref[...] = sum(crossed[h * latents : (h + 1) * latents] for h in range(heads)).astype(bf16)
    ga = jnp.zeros((latents, inner), f32)
    for w in range(ga_ref.shape[0] // latents):
        ga = ga + ga_ref[pl.ds(w * latents, latents), :].astype(f32) * slot_hit(info_ref, w)
    tall = spread_heads(ga)
    grad_weights = nn(values[...], tall.T.astype(bf16))
    row_dot = jnp.sum(attention * grad_weights, axis=0, keepdims=True)
    grad_scores = attention * (grad_weights - row_dot)
    grad_keys = (nn(grad_scores.astype(bf16), q_ref[...]) * 0.125).astype(bf16)
    grad_values = nn(attention_b, tall.astype(bf16)).astype(bf16)
    grads[:, pl.ds(0, inner)] = grad_keys[:tokens]
    grads[:, pl.ds(inner, inner)] = grad_values[:tokens]
    late_rows = [grad_keys[tokens:].astype(f32), grad_values[tokens:].astype(f32)]
    if not first:
        late_rows = [lat_in[:, i * inner : (i + 1) * inner] + late_rows[i] for i in range(2)]
    if not last:
        term = tn(full[pl.ds(0, tokens), :], grads[...])
        acc_ref[...] = term if first else acc_in[...] + term
        lat_ref[:, pl.ds(0, inner)] = late_rows[0]
        lat_ref[:, pl.ds(inner, inner)] = late_rows[1]
        return
    twice = jnp.concatenate([norm_ref[...]] * 2, axis=0)
    for i in range(2):
        columns = slice(i * inner, (i + 1) * inner)
        high = late_rows[i].astype(bf16)
        low = (late_rows[i] - high.astype(f32)).astype(bf16)
        total = tn(full[pl.ds(0, tokens), :], grads[:, columns]) + tn(twice, jnp.concatenate([high, low], axis=0))
        if not first:
            total = total + acc_in[:, columns]
        if split is None:
            done[i][...] = (total * scale).astype(bf16)
            continue
        rows, count, bits = split
        late[...] = total * scale
        bit = bits[i]
        mine = (lax.axis_index("dp") // bit) % 2
        for j in range(count // 2):
            for side in range(2):
                chosen = mine if side == 0 else 1 - mine
                block = (j // bit) * 2 * bit + chosen * bit + j % bit
                at = pl.multiple_of(block * rows, rows)
                done[2 * i + side][pl.ds(j * rows, rows), :] = late[pl.ds(at, rows), :].astype(bf16)


def out_body(work, parts, *refs):
    infos = refs[:work]
    atts = refs[work : 2 * work]
    latents_ref, ow_ref, out_ref, base_ref, rows = refs[2 * work :]
    latents = latents_ref.shape[0]
    width = base_ref.shape[2]
    for p in range(work):
        rows[pl.ds(p * latents, latents), :] = atts[p][...]
    me = lax.axis_index("mp")
    start = pl.multiple_of(me * width, width)
    mine = latents_ref[:, pl.ds(start, width)]
    for j in range(parts):
        part = nn(rows[...], ow_ref[:, j * width : (j + 1) * width])
        for w in range(work):
            value = jnp.zeros((latents, width), f32)
            for p in range(work):
                rows_p = part[p * latents : (p + 1) * latents]
                value = value + rows_p * slot_hit(infos[p], w)
            out_ref[j, pl.ds(w * latents, latents), :] = value.astype(bf16)
    for w in range(work):
        live = jnp.zeros((1, 1), f32)
        for p in range(work):
            live = live + slot_hit(infos[p], w)
        base_ref[w] = mine.astype(f32) * live


def gather_blocks(block, axis):
    size = lax.axis_size(axis)
    blocks = {0: block}
    bit = size // 2
    while bit >= 1:
        for key in list(blocks):
            blocks[key ^ bit] = flip(blocks[key], axis, bit)
        bit //= 2
    return [blocks[b] for b in range(size)]


def pick_side(value, axis, bit_axis, bit):
    mine = (lax.axis_index(axis) // bit) % 2
    keep = lax.dynamic_index_in_dim(value, mine, bit_axis, keepdims=True)
    send = lax.dynamic_index_in_dim(value, 1 - mine, bit_axis, keepdims=True)
    return keep, send


def exchange(keep, send, axis, bit, last):
    got = flip(send, axis, bit)
    total = keep.astype(f32) + got.astype(f32)
    return total if last else total.astype(bf16)


def fold_body(rows, bit, *refs):
    send_ref, keep_ref = refs[4:]
    mine = (lax.axis_index("dp") // bit) % 2
    ours = pl.ds(pl.multiple_of(mine * rows, rows), rows)
    theirs = pl.ds(pl.multiple_of((1 - mine) * rows, rows), rows)
    for i in range(2):
        held, got = refs[2 * i], refs[2 * i + 1]
        out = pl.ds(i * rows, rows)
        keep_ref[out, :] = held[ours, :].astype(f32) + got[ours, :].astype(f32)
        total = held[theirs, :].astype(f32) + got[theirs, :].astype(f32)
        send_ref[out, :] = total.astype(bf16)


def finish_body(keep_ref, got_ref, key_ref, value_ref):
    rows = key_ref.shape[0]
    for i, out in enumerate((key_ref, value_ref)):
        part = pl.ds(i * rows, rows)
        out[...] = keep_ref[part, :] + got_ref[part, :].astype(f32)


def merged_exchange(keeps, sends, rows, inner, bits):
    low, middle, high = bits
    shape = jax.ShapeDtypeStruct
    sides = []
    for keep, send, first, second in (
        (keeps[0], sends[0], low, middle),
        (keeps[1], sends[1], middle, low),
    ):
        part = exchange(keep, send, "dp", first, False).reshape(2, 2, rows, inner)
        keep, send = pick_side(part, "dp", 1, second)
        got = flip(send.reshape(2 * rows, inner), "dp", second)
        sides += [keep.reshape(2 * rows, inner), got]
    send, keep = Chain().call(
        functools.partial(fold_body, rows, high),
        [shape((2 * rows, inner), bf16), shape((2 * rows, inner), f32)],
        [VMEM] * 4,
        [VMEM] * 2,
        sides,
        moved=16 * rows * inner,
        limit=4,
        alone=True,
    )
    return Chain().call(
        finish_body,
        [shape((rows, inner), f32)] * 2,
        [VMEM] * 2,
        [VMEM] * 2,
        (keep, flip(send, "dp", high)),
        moved=16 * rows * inner,
        limit=4,
        alone=True,
    )


def powers(size):
    found = []
    while 2 ** len(found) < size:
        found.append(2 ** len(found))
    return found


def layer(
    media,
    time_table,
    doc_images,
    plan,
    latents,
    queries,
    key_weight,
    value_weight,
    out_weight,
    cotangent,
):
    slots, tokens, width = media.shape
    work, latent_count, _ = cotangent.shape
    reach = slots - work
    model_width = latents.shape[1]
    inner = queries.shape[1]
    heads = inner // HEAD
    cross = heads * latent_count
    parts = lax.axis_size("mp")
    dp = lax.axis_size("dp")
    bits = powers(dp)
    depth = len(bits)
    turned = bits[1:2] + bits[:1] + bits[2:]
    rows = model_width // dp
    shape = jax.ShapeDtypeStruct
    chain = Chain()

    fact_rows = -(-(2 * work + 1) // 8) * 8
    control = jnp.concatenate([plan.reshape(-1), doc_images])
    *sends, own, facts = chain.call(
        functools.partial(prep_body, work, reach),
        [shape((tokens + MARK_ROWS, width), bf16)] * reach
        + [shape((work, tokens, width), bf16), shape((fact_rows, width), f32)],
        [HBM] * 2,
        [VMEM] * (reach + 2),
        (control, media),
        [
            pltpu.SMEM(control.shape, jnp.int32),
            pltpu.SemaphoreType.DMA((reach,)),
            pltpu.SemaphoreType.DMA((work,)),
            pltpu.SemaphoreType.DMA((1,)),
        ],
        moved=(reach + work) * tokens * width * 4,
        full=True,
        spare=SPARE,
    )
    arrivals = []
    for k in range(2, reach + 1):
        arrivals.append(from_behind(sends[k - 1], "dp", k))
    if dp % 2 == 0:
        near = flip(sends[0], "dp", 1)
        route = [(i, i if i % 2 else (i + 2) % dp) for i in range(dp)]
        arrivals.append(lax.ppermute(near, "dp", route))
    else:
        arrivals.append(from_behind(sends[0], "dp", 1))
    cot_blocks = gather_blocks(cotangent.reshape(work * latent_count, width), "mp")
    (table,) = chain.call(
        table_body,
        [shape(time_table.shape, f32)],
        [HBM],
        [VMEM],
        (time_table,),
        [pltpu.VMEM(time_table.shape, bf16), pltpu.SemaphoreType.DMA((1,))],
        limit=1,
    )
    infos = []
    gathered = []
    attended = []
    sums = ()
    shared = ()

    def select(p):
        seen = seen_at(work, reach, p)
        block, info = chain.call(
            functools.partial(select_body, work, reach, p),
            [shape((tokens, width), bf16), shape((8, 128), f32)],
            [VMEM] * (seen + 3),
            [VMEM, VMEM],
            (facts, table, own, *arrivals[:seen]),
            moved=tokens * width * 4,
            limit=2,
        )
        infos.append(info)
        gathered.append(gather_blocks(block, "mp"))

    def place(p):
        nonlocal sums, shared
        first, last = p == 0, p == work - 1
        held_rows = tokens + latent_count
        split = None
        new = [
            shape((model_width, 2 * inner), f32),
            shape((latent_count, 2 * inner), f32),
        ]
        if last:
            if rows % 16 == 0 and depth:
                split = (rows, dp, (bits[0], turned[0]))
                new = [shape((model_width // 2, inner), bf16)] * 4
            else:
                new = [shape((model_width, inner), bf16)] * 2
        scratch = [
            pltpu.VMEM((held_rows if first else tokens, model_width), bf16),
            pltpu.VMEM((held_rows, inner), bf16),
            pltpu.VMEM((held_rows, inner), bf16),
            pltpu.VMEM((tokens, 2 * inner), bf16),
        ]
        args = (infos[p], *gathered[p], key_weight, value_weight)
        extra = []
        if first:
            args += (latents, queries, out_weight, *cot_blocks)
            extra = [
                shape((work * latent_count, inner), bf16),
                shape((latent_count, inner), bf16),
                shape((latent_count, inner), bf16),
                shape((inner, cross), bf16),
                shape((cross, inner), bf16),
                shape((latent_count, model_width), bf16),
            ]
            scratch.append(pltpu.VMEM((work * latent_count, model_width), bf16))
        else:
            args += (*sums, *shared)
        if last:
            scratch.append(pltpu.VMEM((model_width, inner), f32))
        start = 3 + parts
        results = chain.call(
            functools.partial(place_body, parts, first, last, 1.0 / (dp * work), split),
            [*new, shape((latent_count, inner), bf16), *extra],
            [VMEM] * len(args),
            [VMEM] * (len(new) + 1 + len(extra)),
            args,
            scratch,
            flops=8 * tokens * model_width * inner + 14 * held_rows * inner * cross,
            limit=16,
            aliases={} if first or last else {start: 0, start + 1: 1},
        )
        sums = tuple(results[: len(new)])
        attended.append(results[len(new)])
        if first:
            shared = tuple(results[len(new) + 1 :])

    for p in range(work):
        if p == 2:
            place(0)
        select(p)
    for p in range(int(work > 2), work):
        place(p)
    carried = sums

    if depth == 3 and len(carried) == 4:
        key_grad, value_grad = merged_exchange(carried[0::2], carried[1::2], rows, inner, bits)
    else:
        grads = []
        for i, order in enumerate((bits, turned)):
            left = list(reversed(bits))
            if len(carried) == 4:
                keep, send = carried[2 * i : 2 * i + 2]
                left.remove(order[0])
                dims = (2,) * len(left) + (rows, inner)
                part = exchange(keep, send, "dp", order[0], depth == 1).reshape(dims)
                order = order[1:]
            else:
                part = carried[i].reshape((2,) * depth + (rows, inner))
            grads.append([part, left, order])
        for step in range(max((len(g[2]) for g in grads), default=0)):
            for g in grads:
                part, left, order = g
                bit = order[step]
                keep, send = pick_side(part, "dp", left.index(bit), bit)
                part = exchange(keep, send, "dp", bit, step == len(order) - 1)
                left.remove(bit)
                g[0] = part.reshape((2,) * len(left) + (rows, inner))
        key_grad, value_grad = [g[0].astype(f32) for g in grads]

    partial_out, base = chain.call(
        functools.partial(out_body, work, parts),
        [
            shape((parts, work * latent_count, width), bf16),
            shape((work, latent_count, width), f32),
        ],
        [VMEM] * (2 * work + 2),
        [VMEM] * 2,
        (*infos, *attended, latents, out_weight),
        [pltpu.VMEM((work * latent_count, inner), bf16)],
        flops=2 * work * latent_count * inner * model_width,
        limit=8,
    )
    out_bits = powers(parts)
    out = partial_out.reshape((2,) * len(out_bits) + partial_out.shape[1:])
    for step, bit in enumerate(out_bits):
        keep, send = pick_side(out, "mp", len(out_bits) - 1 - step, bit)
        out = exchange(keep, send, "mp", bit, step == len(out_bits) - 1)
    resampled = (base + out.reshape(base.shape)).astype(bf16)
    return (resampled, key_grad, value_grad)


def solution(mesh):
    return jax.shard_map(
        layer,
        mesh=mesh,
        in_specs=(
            P("dp", None, "mp"),
            P(None, "mp"),
            P("dp"),
            P("dp", None),
            P(),
            P(None, "mp"),
            P(None, "mp"),
            P(None, "mp"),
            P("mp", None),
            P("dp", None, "mp"),
        ),
        out_specs=(P("dp", None, "mp"), P("dp", "mp"), P("dp", "mp")),
        check_vma=False,
    )
```
